128 devices in a mesh: ctx: 16 (over z, y_lo, core), tp: 8 (over y_hi, x).
Axes of the slice: x: 4, y: 4 (y_hi: 2, y_lo: 2; y = y_hi * 2 + y_lo), z: 4, core: 2. Of those that a mesh axis runs over, the one named last changes fastest.
Arguments:
- inner_x: bfloat16 [2, 2048, 16384], P(None, 'ctx', 'tp'), may hold values from -6 to 6
- gate_z: bfloat16 [2, 2048, 16384], P(None, 'ctx', 'tp'), may hold values from -6 to 6
- proj_bc: bfloat16 [2, 2048, 8, 512], P(None, 'ctx', 'tp'), may hold values from -6 to 6
- dt_raw: float32 [2, 256, 2048], P(None, 'tp', 'ctx'), may hold values from -6 to 82
- a_log: float32 [256], P('tp'), may hold values from -10 to 1
- dt_bias: float32 [256], P('tp'), may hold values from -0.5 to 0.5
- d_skip: float32 [256], P('tp'), may hold values from 0.5 to 1.5
- conv_x: float32 [4, 16384], P(None, 'tp'), may hold values from -3 to 3
- conv_bc: float32 [4, 8, 512], P(None, 'tp'), may hold values from -3 to 3
- bias_x: float32 [16384], P('tp'), may hold values from -0.5 to 0.5
- bias_bc: float32 [8, 512], P('tp'), may hold values from -0.5 to 0.5
- norm_gain: float32 [16384], P('tp'), may hold values from 0.25 to 1.75
- init_state: float32 [2, 256, 64, 256], P(None, 'tp'), may hold values from -6 to 6
- init_conv_x: bfloat16 [2, 3, 16384], P(None, None, 'tp'), may hold values from -6 to 6
- init_conv_bc: bfloat16 [2, 3, 8, 512], P(None, None, 'tp'), may hold values from -6 to 6
- lengths: int32 [2], replicated, may hold values from 1024 to 2048, as said below
- dec_x: bfloat16 [4, 128, 16384], P(None, 'ctx', 'tp'), may hold values from -6 to 6
- dec_z: bfloat16 [4, 128, 16384], P(None, 'ctx', 'tp'), may hold values from -6 to 6
- dec_bc: bfloat16 [4, 128, 8, 512], P(None, 'ctx', 'tp'), may hold values from -6 to 6
- dec_dt: float32 [4, 256, 128], P(None, 'tp', 'ctx'), may hold values from -2.5 to 1
- row_prompt: int32 [128], P('ctx'), may hold values from 0 to 1
- w_out: bfloat16 [16384, 8192], P('tp', 'ctx'), may hold values from -0.046875 to 0.046875
Outputs:
- prefill_out: bfloat16 [2, 2048, 16384], P(None, 'ctx', 'tp')
- layer_out: bfloat16 [4, 128, 8192], P(None, 'tp', 'ctx')
The draws below stay inside these ranges and needn't reach their ends.
Inputs may be any that keep to these rules, and one draw needn't show every extreme that they name: Positions from lengths[s] on are padding of prompt s. At least one prompt has all 2048 positions live.
All inputs are finite; a program needn't handle non-finite values.
Results may differ from the reference program's by a relative error of at most 0.005.
Values may be sent and summed in bfloat16 or wider, within the bound.
A program may use at most 256 MiB of HBM per device.

```python
import math
import jax
import jax.numpy as jnp
from jax import lax

D = 8192
HEADS = 256
HEAD_DIM = 64
STATE = 256
GROUPS = 8
CONV_K = 4
SEQS = 2
TOK_DEV = 128
STEPS = 4
INNER = 16384
LENGTH = 2048
ROWS = 128


def draw_a_log(key, part):
    first, second, third = jax.random.split(jax.random.fold_in(key, 11), 3)
    share = 0.6
    slow = jax.random.uniform(first, (HEADS,)) < share
    slow_rate = jnp.exp(jax.random.uniform(second, (HEADS,), minval=jnp.log(0.05), maxval=jnp.log(0.3))) / (0.02 * LENGTH)
    fast_rate = jax.random.uniform(third, (HEADS,), minval=1.0, maxval=1.65)
    return jnp.log(jnp.where(slow, slow_rate, fast_rate)).astype(jnp.float32)


def draw_dt_raw(key, part):
    first, second, third, fourth = jax.random.split(jax.random.fold_in(key, 23), 4)
    spread = 0.7
    noise = jax.random.uniform(first, (SEQS, HEADS, LENGTH), minval=-spread, maxval=spread)
    blocks = LENGTH // TOK_DEV
    offset = jnp.repeat(jax.random.uniform(second, (SEQS, HEADS, blocks), minval=-0.35, maxval=0.35), TOK_DEV, axis=2)
    places = jax.random.randint(third, (SEQS, 3), 0, LENGTH)
    spot = jnp.any(jnp.arange(LENGTH)[None, None, :] == places[:, :, None], axis=1)
    height = 0.02 * LENGTH * (1.0 + jax.random.uniform(fourth, (SEQS, 1, LENGTH)))
    base = -3.9 + noise + offset
    return jnp.where(spot[:, None, :], height, base).astype(jnp.float32)


def draw_lengths(key, part):
    first, second = jax.random.split(jax.random.fold_in(key, 31), 2)
    full_one = jax.random.randint(first, (), 0, SEQS)
    others = jax.random.randint(second, (SEQS,), LENGTH // 2, LENGTH + 1)
    chosen = jnp.arange(SEQS, dtype=jnp.int32) == full_one
    return jnp.where(chosen, LENGTH, others).astype(jnp.int32)


def with_ends(entries, key, low, top_value):
    index_at = [jax.random.randint(jax.random.fold_in(key, axis), (), 0, length) for axis, length in enumerate(entries.shape)]
    widest = entries.shape.index(max(entries.shape))
    beside = index_at[:widest] + [(index_at[widest] + 1) % entries.shape[widest]] + index_at[widest + 1:]
    return entries.at[tuple(index_at)].set(low).at[tuple(beside)].set(top_value)


def level_of(own_key, dims, cuts, least, largest):
    factor_of, own = 1.0, jax.random.fold_in(own_key, 6)
    for axis_at, parts in cuts:
        heights = jnp.exp(jax.random.uniform(jax.random.fold_in(own, axis_at), (parts,), jnp.float32, least / len(cuts), largest / len(cuts)))
        factor_of = factor_of * jnp.repeat(heights, dims[axis_at] // parts).reshape([-1 if axis == axis_at else 1 for axis in range(len(dims))])
    return factor_of


def bell_draw(own_key, shape, deviation, most, cuts=(), kind=jnp.bfloat16):
    values = deviation * jax.random.normal(own_key, shape, jnp.float32)
    if cuts:
        values = values * level_of(own_key, shape, cuts, -0.22, 0.18)
    return jnp.clip(values, -most, most).astype(kind)


def setup_inputs(seed: int = 0) -> dict:
    streams_of = jax.random.split(jax.random.key(seed), 23)
    inner_x = bell_draw(streams_of[0], (SEQS, LENGTH, INNER), 1.0, 6.0, ((1, 16), (2, 8)))
    gate_z = bell_draw(streams_of[1], (SEQS, LENGTH, INNER), 1.0, 6.0, ((1, 16), (2, 8)))
    proj_bc = bell_draw(streams_of[2], (SEQS, LENGTH, GROUPS, 2 * STATE), 1.0, 6.0, ((1, 16), (2, 8)))
    dt_raw = draw_dt_raw(jax.random.fold_in(streams_of[22], 71), 0)
    a_log = draw_a_log(jax.random.fold_in(streams_of[22], 71), 0)
    dt_bias = jnp.clip(jax.random.uniform(streams_of[5], (HEADS,), jnp.float32, -0.5, 0.5) * level_of(streams_of[5], (HEADS,), ((0, 8),), -0.4, 0.0), -0.5, 0.5)
    d_skip = jnp.clip(0.5 + 1.0 * jax.random.uniform(streams_of[6], (HEADS,), jnp.float32) ** level_of(streams_of[6], (HEADS,), ((0, 8),), -0.2, 0.2), 0.5, 1.5)
    conv_x = bell_draw(streams_of[7], (CONV_K, INNER), CONV_K ** -0.5, 3.0, ((1, 8),), jnp.float32)
    conv_bc = bell_draw(streams_of[8], (CONV_K, GROUPS, 2 * STATE), CONV_K ** -0.5, 3.0, ((1, 8),), jnp.float32)
    bias_x = jnp.clip(jax.random.uniform(streams_of[9], (INNER,), jnp.float32, -0.5, 0.5) * level_of(streams_of[9], (INNER,), ((0, 8),), -0.4, 0.0), -0.5, 0.5)
    bias_bc = jnp.clip(jax.random.uniform(streams_of[10], (GROUPS, 2 * STATE), jnp.float32, -0.5, 0.5) * level_of(streams_of[10], (GROUPS, 2 * STATE), ((0, 8),), -0.4, 0.0), -0.5, 0.5)
    norm_gain = jnp.clip(1.0 + 0.15 * jax.random.normal(streams_of[11], (INNER,), jnp.float32), 0.25, 1.75)
    init_state = bell_draw(streams_of[12], (SEQS, HEADS, HEAD_DIM, STATE), 1.0, 6.0, ((1, 8),), jnp.float32)
    init_conv_x = bell_draw(streams_of[13], (SEQS, CONV_K - 1, INNER), 1.0, 6.0, ((2, 8),))
    init_conv_bc = bell_draw(streams_of[14], (SEQS, CONV_K - 1, GROUPS, 2 * STATE), 1.0, 6.0, ((2, 8),))
    lengths = draw_lengths(jax.random.fold_in(streams_of[22], 71), 0)
    dec_x = bell_draw(streams_of[16], (STEPS, ROWS, INNER), 1.0, 6.0, ((1, 16), (2, 8)))
    dec_z = bell_draw(streams_of[17], (STEPS, ROWS, INNER), 1.0, 6.0, ((1, 16), (2, 8)))
    dec_bc = bell_draw(streams_of[18], (STEPS, ROWS, GROUPS, 2 * STATE), 1.0, 6.0, ((1, 16), (2, 8)))
    dec_dt = jnp.clip(-2.5 + 3.5 * jax.random.uniform(streams_of[19], (STEPS, HEADS, ROWS), jnp.float32) ** level_of(streams_of[19], (STEPS, HEADS, ROWS), ((1, 8), (2, 16)), -0.2, 0.2), -2.5, 1.0)
    row_prompt = with_ends(jax.random.randint(streams_of[20], (ROWS,), 0, SEQS), jax.random.fold_in(streams_of[20], 1), 0, SEQS - 1).astype(jnp.int32)
    w_out = bell_draw(streams_of[21], (INNER, D), INNER ** -0.5, 0.046875, ((0, 8), (1, 16)))
    return dict(inner_x=inner_x, gate_z=gate_z, proj_bc=proj_bc, dt_raw=dt_raw, a_log=a_log, dt_bias=dt_bias, d_skip=d_skip, conv_x=conv_x, conv_bc=conv_bc, bias_x=bias_x, bias_bc=bias_bc, norm_gain=norm_gain, init_state=init_state, init_conv_x=init_conv_x, init_conv_bc=init_conv_bc, lengths=lengths, dec_x=dec_x, dec_z=dec_z, dec_bc=dec_bc, dec_dt=dec_dt, row_prompt=row_prompt, w_out=w_out)


epsilon = 1e-05
highest = lax.Precision.HIGHEST

def gated_norm(values, gate, gain):
    mixed = values * jax.nn.silu(gate)
    shape = mixed.shape
    grouped = mixed.reshape(shape[:-1] + (GROUPS, shape[-1] // GROUPS))
    scaled = grouped * lax.rsqrt(lax.optimization_barrier(jnp.mean(grouped * grouped, axis=-1, keepdims=True)) + epsilon)
    return scaled.reshape(shape) * gain

def prefill_prompt(inner_row, gate_row, bc_row, raw_rate, start_state, start_x, start_bc, length, a_log, dt_bias, d_skip, tap_weights, tap_bias, norm_gain):
    head_part = jnp.concatenate([start_x, start_bc.reshape(CONV_K - 1, -1)], axis=-1)
    body_part = jnp.concatenate([inner_row, bc_row.reshape(LENGTH, -1)], axis=-1)
    raw = jnp.concatenate([head_part, body_part], axis=0)
    padded = raw.astype(jnp.float32)
    total = tap_bias
    for offset in range(CONV_K):
        total = total + tap_weights[offset] * padded[offset:offset + LENGTH]
    active = jax.nn.silu(total)
    per_group = HEADS // GROUPS
    block = math.gcd(LENGTH, 256)
    count = LENGTH // block
    values = active[:, :INNER].reshape(count, block, GROUPS, per_group, HEAD_DIM)
    mixers = active[:, INNER:].reshape(count, block, GROUPS, 2 * STATE)
    live = (jnp.arange(LENGTH, dtype=jnp.int32) < length).astype(jnp.float32)
    rate = jnp.exp(a_log)
    step_size = jax.nn.softplus(raw_rate + dt_bias[:, None]) * live[None, :]
    log_decay = -rate[:, None] * step_size
    step_blocks = step_size.reshape(GROUPS, per_group, count, block).transpose(2, 0, 1, 3)
    decay_blocks = log_decay.reshape(GROUPS, per_group, count, block).transpose(2, 0, 1, 3)
    lower = jnp.arange(block)[:, None] >= jnp.arange(block)[None, :]
    skip_group = d_skip.reshape(GROUPS, per_group)

    def advance(state, items):
        value_block, mixer_block, step_block, decay_block = items
        b_part = mixer_block[..., :STATE]
        c_part = mixer_block[..., STATE:]
        running = jnp.cumsum(decay_block, axis=-1)
        scores = jnp.einsum('tgn,ugn->gtu', c_part, b_part, precision=highest)
        gap = running[..., :, None] - running[..., None, :]
        mixing = jnp.where(lower, jnp.exp(jnp.where(lower, gap, 0.0)), 0.0) * scores[:, None] * step_block[..., None, :]
        y_local = jnp.einsum('ghtu,ughp->tghp', mixing, value_block, precision=highest)
        y_carried = jnp.einsum('tgn,ghpn->tghp', c_part, state, precision=highest) * jnp.exp(jnp.transpose(running, (2, 0, 1)))[..., None]
        to_end = jnp.exp(running[..., -1:] - running) * step_block
        weighted = value_block * jnp.transpose(to_end, (2, 0, 1))[..., None]
        new_state = jnp.exp(running[..., -1])[..., None, None] * state + jnp.einsum('ughp,ugn->ghpn', weighted, b_part, precision=highest)
        return (new_state, y_local + y_carried + skip_group[:, :, None] * value_block)
    final, outputs = lax.scan(advance, start_state.reshape(GROUPS, per_group, HEAD_DIM, STATE), (values, mixers, step_blocks, decay_blocks))
    mixed_y = outputs.reshape(LENGTH, INNER)
    result = gated_norm(mixed_y, gate_row.astype(jnp.float32), norm_gain).astype(jnp.bfloat16)
    tail = lax.dynamic_slice_in_dim(raw, length.astype(jnp.int32), CONV_K - 1, 0).astype(jnp.float32)
    return (result, final, tail)

def reference(inner_x, gate_z, proj_bc, dt_raw, a_log, dt_bias, d_skip, conv_x, conv_bc, bias_x, bias_bc, norm_gain, init_state, init_conv_x, init_conv_bc, lengths, dec_x, dec_z, dec_bc, dec_dt, row_prompt, w_out):
    tap_weights = jnp.concatenate([conv_x, conv_bc.reshape(CONV_K, -1)], axis=-1)
    tap_bias = jnp.concatenate([bias_x, bias_bc.reshape(-1)], axis=-1)
    results, finals, tails = ([], [], [])
    for prompt in range(SEQS):
        result, final, tail = prefill_prompt(inner_x[prompt], gate_z[prompt], proj_bc[prompt], dt_raw[prompt], init_state[prompt], init_conv_x[prompt], init_conv_bc[prompt], lengths[prompt], a_log, dt_bias, d_skip, tap_weights, tap_bias, norm_gain)
        results.append(result)
        finals.append(final)
        tails.append(tail)
    prefill_out = jnp.stack(results)
    final_all = jnp.stack(finals)
    tail_all = jnp.stack(tails)
    per_group = HEADS // GROUPS
    rate_group = jnp.exp(a_log).reshape(GROUPS, per_group)
    skip_group = d_skip.reshape(GROUPS, per_group)

    def decode_row(items):
        prompt, row_x, row_z, row_bc, row_dt = items
        state = lax.dynamic_index_in_dim(final_all, prompt.astype(jnp.int32), 0, keepdims=False)
        window = lax.dynamic_index_in_dim(tail_all, prompt.astype(jnp.int32), 0, keepdims=False)
        hidden = []
        for moment in range(STEPS):
            fresh = jnp.concatenate([row_x[moment], row_bc[moment].reshape(-1)]).astype(jnp.float32)
            full = jnp.concatenate([window, fresh[None]], axis=0)
            total = tap_bias
            for offset in range(CONV_K):
                total = total + tap_weights[offset] * full[offset]
            active = jax.nn.silu(total)
            values = active[:INNER].reshape(GROUPS, per_group, HEAD_DIM)
            mixers = active[INNER:].reshape(GROUPS, 2 * STATE)
            step_row = jax.nn.softplus(row_dt[moment] + dt_bias).reshape(GROUPS, per_group)
            keep = jnp.exp(-rate_group * step_row)
            state = keep[..., None, None] * state + (step_row[..., None] * values)[..., None] * mixers[:, None, None, :STATE]
            y_row = jnp.einsum('ghpn,gn->ghp', state, mixers[:, STATE:], precision=highest) + skip_group[:, :, None] * values
            hidden.append(gated_norm(y_row.reshape(INNER), row_z[moment].astype(jnp.float32), norm_gain).astype(jnp.bfloat16))
            window = full[1:]
        return jnp.stack(hidden)
    hidden_rows = lax.map(decode_row, (row_prompt, jnp.transpose(dec_x, (1, 0, 2)), jnp.transpose(dec_z, (1, 0, 2)), jnp.transpose(dec_bc, (1, 0, 2, 3)), jnp.transpose(dec_dt, (2, 0, 1))))
    dec_hidden = jnp.transpose(hidden_rows, (1, 0, 2))
    layer_out = jnp.dot(dec_hidden.reshape(-1, INNER), w_out, preferred_element_type=jnp.float32)
    return (prefill_out, layer_out.reshape(STEPS, ROWS, D).astype(jnp.bfloat16))
```

```python
import functools

import jax
import jax.numpy as jnp
from jax import lax
from jax.experimental import pallas as pl
from jax.experimental.pallas import tpu as pltpu
from jax.sharding import PartitionSpec as P

MESH = pl.DeviceIdType.MESH
F32, BF16 = jnp.float32, jnp.bfloat16
HIGH = lax.Precision.HIGHEST
LANES = 128
CHIPS, CTX, TP = 8, 16, 8


def split(v):
    high = v.astype(BF16)
    return high, (v - high.astype(F32)).astype(BF16)


def dot(a, b):
    return jnp.dot(a, b, preferred_element_type=F32)


def silu(v):
    return v / (1.0 + jnp.exp(-v))


def softplus(v):
    return jnp.maximum(v, 0.0) + jnp.log1p(jnp.exp(-jnp.abs(v)))


def kernel(
    x_ref, bc_ref, z_hbm, dt_ref, par_ref, pbc_ref, hp_ref, init_hbm, rim0_ref,
    dx_ref, dz_ref, dbc_ref, sm_ref, len_ref, w_hbm,
    pre_ref, lay_ref,
    zbuf, ibuf, wbuf, rimsend, rimrecv, rimf, tailx, tailbc,
    dxr, dzr, dbcr, smr, txr, tbr,
    runrows, cols, bthl, chl, scs, dall, drecv, dstage, dchip,
    osend, oown, orecv, ostage, arecv, est, retst, erecv, e2send, e2recv,
    vp, er, yacc, ssqp, gbuf, ssqs, ssqr, flat, fstage, rbuf,
    lsem, rims, rimr, decs, decr, d2s, d2r, dds, ddr, as_, ar, ads, adr,
    rs_, rr, e2s, e2r, gs, gr, gfs, gfr, qs, qr, ts, tr,
):
    c, t = lax.axis_index("ctx"), lax.axis_index("tp")
    q, core = lax.div(c, 2), lax.rem(c, 2)
    mate = q * 2 + (1 - core)
    blk = core * CHIPS + q
    prompts, tokens, width = x_ref.shape
    tiles = width // LANES
    states = init_hbm.shape[3]
    steps, batch = dx_ref.shape[:2]
    rows = batch * CTX

    def lanes_of(j, size=LANES):
        return pl.ds(pl.multiple_of(j * size, size), size)

    def remote(src, dst, ssem, rsem, ctx=None, tp=None):
        return pltpu.make_async_remote_copy(
            src_ref=src, dst_ref=dst, send_sem=ssem, recv_sem=rsem,
            device_id=(c if ctx is None else ctx, t if tp is None else tp),
            device_id_type=MESH,
        )

    zcopy = pltpu.make_async_copy(z_hbm, zbuf, lsem.at[0])
    icopy = pltpu.make_async_copy(init_hbm.at[:, blk], ibuf, lsem.at[1])
    wcopy = pltpu.make_async_copy(w_hbm, wbuf, lsem.at[2])
    zcopy.start()
    icopy.start()
    wcopy.start()

    ends = [x_ref[s, tokens - 16 :, :].astype(F32)[8:] for s in range(prompts)]
    rimsend[:, :width] = jnp.concatenate(ends, 0).astype(BF16)
    ends = [bc_ref[s, tokens - 16 :, :].astype(F32)[8:] for s in range(prompts)]
    rimsend[:, width:] = jnp.concatenate(ends, 0).astype(BF16)
    place = lax.broadcasted_iota(jnp.int32, (8, tokens), 1) + c * tokens
    slot = lax.broadcasted_iota(jnp.int32, (8, tokens), 0)
    tx, tbc = [], []
    for s in range(prompts):
        hit = (place == len_ref[s] - 3 + slot) & (slot < 3)
        pick = jnp.where(hit, 1.0, 0.0).astype(BF16)
        tx.append(dot(pick, x_ref[s]))
        tbc.append(dot(pick, bc_ref[s]))
    tailx[...] = jnp.concatenate(tx, 0).astype(BF16)
    tailbc[...] = jnp.concatenate(tbc, 0).astype(BF16)
    dxr[:, c] = dx_ref[:, :, lanes_of(blk)]
    dzr[:, c] = dz_ref[:, :, lanes_of(blk)]
    dbcr[:, c] = dbc_ref[...]
    smr[c] = sm_ref[...]
    txr[c] = tailx[:, lanes_of(blk)]
    tbr[c] = tailbc[...]
    dall[...] = jnp.zeros_like(dall)
    dstage[...] = jnp.zeros_like(dstage)

    barrier = pltpu.get_barrier_semaphore()
    for k in range(1, CTX):
        pl.semaphore_signal(barrier, inc=1, device_id=(lax.rem(c + k, CTX), t), device_id_type=MESH)
    for k in range(1, TP):
        pl.semaphore_signal(barrier, inc=1, device_id=(c, lax.rem(t + k, TP)), device_id_type=MESH)
    pl.semaphore_wait(barrier, CTX - 1 + TP - 1)

    rim = remote(rimsend, rimrecv, rims, rimr, ctx=lax.rem(c + 1, CTX))
    rim.start()

    def decode_copies(k, source):
        to = lax.rem(c + k, CTX)
        their = lax.rem(to, 2) * CHIPS + lax.div(to, 2)
        at = lax.rem(c + CTX - k, CTX) if source else c
        pairs = (
            (dx_ref.at[:, :, lanes_of(their)], dxr.at[:, at]),
            (dz_ref.at[:, :, lanes_of(their)], dzr.at[:, at]),
            (dbc_ref, dbcr.at[:, at]),
            (sm_ref, smr.at[at]),
            (tailx.at[:, lanes_of(their)], txr.at[at]),
            (tailbc, tbr.at[at]),
        )
        return [
            remote(src, dst, decs.at[i, k], decr.at[i, k], ctx=to)
            for i, (src, dst) in enumerate(pairs)
        ]

    @pl.loop(1, CTX)
    def _(k):
        for copy in decode_copies(k, False):
            copy.start()

    upto = lax.broadcasted_iota(jnp.int32, (tokens, tokens), 0)
    at_lane = lax.broadcasted_iota(jnp.int32, (tokens, tokens), 1)
    upper = jnp.where(upto <= at_lane, 1.0, 0.0)
    lower = upto >= at_lane
    heads = dt_ref.shape[1]
    lane_place = lax.broadcasted_iota(jnp.int32, (heads, tokens), 1) + c * tokens
    for s in range(prompts):
        live = lane_place < len_ref[s]
        step = jnp.where(live, softplus(dt_ref[s] + hp_ref[1]), 0.0)
        run = jnp.dot(-hp_ref[0] * step, upper, precision=HIGH, preferred_element_type=F32)
        runrows[s] = run
        both = jnp.concatenate([run, step, jnp.zeros((tokens - 2 * heads, tokens), F32)], 0)
        cols[s] = both.T

    rim.wait_recv()
    rimf[...] = jnp.where(c == 0, rim0_ref[...], rimrecv[...].astype(F32))

    def conv(rim_rows, body, taps):
        padded = jnp.concatenate([rim_rows, body], 0)
        total = taps[4:5]
        for k in range(4):
            total = total + taps[k : k + 1] * padded[5 + k : 5 + k + body.shape[0]]
        return silu(total)

    for s in range(prompts):
        act = conv(rimf[8 * s : 8 * s + 8, width:], bc_ref[s].astype(F32), pbc_ref[...])
        b, cc = act[:, :states], act[:, states:]
        bt = b.T
        high, low = split(bt)
        bthl[s] = jnp.concatenate([high, low], 1)
        chl[s] = jnp.concatenate(split(cc), 0)
        scores = jnp.dot(cc, bt, precision=HIGH, preferred_element_type=F32)
        scs[s] = jnp.where(lower, scores, 0.0)

    first_half = lax.broadcasted_iota(jnp.int32, (tokens, LANES), 1) < LANES // 2

    def columns(s, j):
        return pltpu.roll(cols[s], lax.rem(tokens - 2 * j, tokens), 1)

    def own_part(j, i, out):
        lanes = lanes_of(j)
        par = par_ref[:, lanes]
        for s in range(prompts):
            xv = conv(rimf[8 * s : 8 * s + 8, lanes], x_ref[s, :, lanes].astype(F32), par)
            col = columns(s, j)
            r = jnp.where(first_half, col[:, 0:1], col[:, 1:2])
            step = jnp.where(first_half, col[:, heads : heads + 1], col[:, heads + 1 : heads + 2])
            end = r[tokens - 1 : tokens]
            v = xv * step
            vp[s, j] = v
            er[s, j] = jnp.exp(r)
            yacc[s, j] = par[6:7] * xv
            dall[s : s + 1, lanes] = jnp.exp(end)
            high, low = split(v * jnp.exp(end - r))
            out[i, s] = dot(bthl[s], jnp.concatenate([high, high], 0)) + dot(
                bthl[s, :, :tokens], low
            )

    def chip_at(k):
        return lax.rem(q + k, CHIPS)

    @pl.loop(1, CHIPS + 1)
    def _(k):
        i = chip_at(k)
        own_part((1 - core) * CHIPS + i, i, osend)
        remote(osend.at[i], orecv.at[i], d2s.at[i], d2r.at[i], ctx=mate).start()

    half = CHIPS * LANES
    dsend = remote(dall.at[:, lanes_of(1 - core, half)], drecv, dds, ddr, ctx=mate)
    dsend.start()

    @pl.loop(1, CHIPS + 1)
    def _(k):
        i = chip_at(k)
        own_part(core * CHIPS + i, i, oown)

    dsend.wait_recv()
    is_first = core == 0

    def decays(s, i):
        own = dall[s : s + 1, lanes_of(core * CHIPS + i)]
        return own, drecv[s : s + 1, lanes_of(i)]

    @pl.loop(1, CHIPS + 1)
    def _(k):
        i = chip_at(k)
        remote(osend.at[i], orecv.at[i], d2s.at[i], d2r.at[i], ctx=mate).wait_recv()
        for s in range(prompts):
            down, theirs = decays(s, i)
            a = jnp.where(is_first, theirs, 1.0)
            b = jnp.where(is_first, 1.0, down)
            ostage[i, s] = (a * oown[i, s] + b * orecv[i, s]).astype(BF16)
            dstage[i, s : s + 1] = down * theirs

        @pl.when(k < CHIPS)
        def _():
            to = i * 2 + core
            remote(ostage.at[i], arecv.at[q], as_.at[k], ar.at[k], ctx=to).start()
            remote(dstage.at[i], dchip.at[q], ads.at[k], adr.at[k], ctx=to).start()

    arecv[q] = ostage[q]
    dchip[q] = dstage[q]

    @pl.loop(0, tiles)
    def _(j):
        for s in range(prompts):
            col = columns(s, j)
            mixing = []
            for h in range(2):
                row = runrows[s, pl.ds(2 * j + h, 1), :]
                gap = jnp.minimum(col[:, h : h + 1] - row, 0.0)
                mixing.append((jnp.exp(gap) * scs[s]).astype(BF16))
            both = jnp.concatenate(mixing, 1)
            v = vp[s, j]
            total = yacc[s, j]
            stacked = jnp.concatenate([jnp.where(first_half, v, 0.0), jnp.where(first_half, 0.0, v)], 0)
            for part in split(stacked):
                total = total + dot(both, part)
            yacc[s, j] = total

    icopy.wait()
    for s in range(prompts):
        est[s] = ibuf[s].T

    @pl.loop(0, CHIPS)
    def _(p):
        for s in range(prompts):
            retst[p, s] = est[s].astype(BF16)
        k = lax.rem(q - p + CHIPS, CHIPS)

        @pl.when(p != q)
        def _():
            back = lax.rem(p - q + CHIPS, CHIPS)
            to = p * 2 + core
            remote(retst.at[p], erecv.at[q], rs_.at[back], rr.at[back], ctx=to).start()
            remote(ostage.at[p], arecv.at[p], as_.at[k], ar.at[k], ctx=to).wait_recv()
            remote(dstage.at[p], dchip.at[p], ads.at[k], adr.at[k], ctx=to).wait_recv()

        for s in range(prompts):
            est[s] = dchip[p, s : s + 1] * est[s] + arecv[p, s].astype(F32)

    erecv[q] = retst[q]

    @pl.loop(1, CTX)
    def _(k):
        for copy in decode_copies(k, True):
            copy.wait_recv()

    par = par_ref[:, lanes_of(blk)]
    small = jnp.concatenate(
        [smr[:, i].reshape(rows, LANES) for i in range(2)], 1
    )
    second = small[:, LANES : LANES + 1] > 0.5
    rolled = pltpu.roll(small[:, :LANES], lax.rem(LANES - 2 * blk, LANES), 1)

    def total_of(ref, lanes):
        out = ref[0].astype(F32)
        for i in range(1, CTX):
            out = out + ref[i].astype(F32)
        return [jnp.where(second, out[8 + k : 9 + k], out[k : k + 1]) for k in range(3)]

    def flat_rows(ref, i):
        return ref[i].astype(F32).reshape(rows, ref.shape[3])

    seq_x = total_of(txr, LANES) + [flat_rows(dxr, i) for i in range(steps)]
    seq_b = total_of(tbr, 2 * states) + [flat_rows(dbcr, i) for i in range(steps)]

    def taps_on(seq, i, weights):
        total = weights[4:5]
        for k in range(4):
            total = total + weights[k : k + 1] * seq[i + k]
        return silu(total)

    final = [split(est[s]) for s in range(prompts)]
    bs, us, coefs = [], [], []
    grown = 1.0
    row8 = lax.broadcasted_iota(jnp.int32, (8, LANES), 0)
    squares = jnp.zeros((8, rows), F32)
    for i in range(steps):
        xd = taps_on(seq_x, i, par)
        bcd = taps_on(seq_b, i, pbc_ref[...])
        cd = bcd[:, states:]
        chigh, clow = split(cd)
        lane = first_half[:rows]
        step = jnp.where(lane, rolled[:, heads * i : heads * i + 1], rolled[:, heads * i + 1 : heads * i + 2])
        keep = jnp.exp(-par[7:8] * step)
        grown = grown * keep
        bs.append(bcd[:, :states])
        us = [keep * u for u in us] + [step * xd]
        y0 = [
            dot(chigh, high) + dot(clow, high) + dot(chigh, low) for high, low in final
        ]
        yd = grown * jnp.where(second, y0[1], y0[0]) + par[6:7] * xd
        for b, u in zip(bs, us):
            yd = yd + u * jnp.sum(b * cd, axis=1, keepdims=True)
        m = yd * silu(flat_rows(dzr, i))
        squares = squares + lax.dot_general(
            jnp.where(row8 == i, 1.0, 0.0), m * m, (((1,), (1,)), ((), ())),
            precision=HIGH, preferred_element_type=F32,
        )
        gbuf[lax.div(blk, 2), i * rows : (i + 1) * rows, lanes_of(lax.rem(blk, 2))] = (
            m * par[5:6]
        ).astype(BF16)
    ssqs[...] = squares
    ssqr[c] = squares

    def slab(chip, which):
        at = which * CHIPS + chip
        return gbuf.at[lax.div(at, 2), :, lanes_of(lax.rem(at, 2))]

    def gather_copy(k, source):
        at = lax.rem(q + CHIPS - k, CHIPS) if source else q
        to = lax.rem(q + k, CHIPS) * 2 + core
        return remote(slab(q, core), slab(at, core), gs.at[k], gr.at[k], ctx=to)

    def forward_copy(k, chip, source):
        which = 1 - core if source else core
        return remote(slab(chip, core), slab(chip, which), gfs.at[k], gfr.at[k], ctx=mate)

    def square_copy(k, source):
        at = lax.rem(c + CTX - k, CTX) if source else c
        return remote(ssqs, ssqr.at[at], qs.at[k], qr.at[k], ctx=lax.rem(c + k, CTX))

    forward_copy(0, q, False).start()

    @pl.loop(1, CHIPS)
    def _(k):
        gather_copy(k, False).start()

    @pl.loop(1, CTX)
    def _(k):
        square_copy(k, False).start()

    zcopy.wait()
    ssqp[...] = jnp.zeros_like(ssqp)

    def finish(s, j, entry):
        carried = dot(chl[s], entry)
        y = yacc[s, j] + (carried[:tokens] + carried[tokens:]) * er[s, j]
        m = y * silu(zbuf[s, :, lanes_of(j)].astype(F32))
        yacc[s, j] = m
        ssqp[s] += m * m

    @pl.loop(0, CHIPS)
    def _(k):
        i = lax.rem(q + CHIPS - k, CHIPS)

        @pl.when(k > 0)
        def _():
            remote(retst.at[i], erecv.at[i], rs_.at[k], rr.at[k], ctx=i * 2 + core).wait_recv()

        mine = []
        for s in range(prompts):
            down, theirs = decays(s, i)
            e = erecv[i, s].astype(F32)
            e2send[i, s] = jnp.where(is_first, down * e + oown[i, s], e).astype(BF16)
            mine.append(jnp.where(is_first, e, theirs * e + orecv[i, s]).astype(BF16))
        remote(e2send.at[i], e2recv.at[i], e2s.at[i], e2r.at[i], ctx=mate).start()
        for s in range(prompts):
            finish(s, core * CHIPS + i, mine[s])

    @pl.loop(0, CHIPS)
    def _(k):
        i = lax.rem(q + CHIPS - k, CHIPS)
        remote(e2send.at[i], e2recv.at[i], e2s.at[i], e2r.at[i], ctx=mate).wait_recv()
        for s in range(prompts):
            finish(s, (1 - core) * CHIPS + i, e2recv[i, s])

    @pl.loop(1, CHIPS)
    def _(k):
        gather_copy(k, True).wait_recv()
        forward_copy(k, lax.rem(q + CHIPS - k, CHIPS), False).start()

    for s in range(prompts):
        mean = jnp.sum(ssqp[s], axis=1, keepdims=True) * (1.0 / width)
        ssqp[s] = jnp.broadcast_to(lax.rsqrt(mean + 1e-5), ssqp.shape[1:])

    @pl.loop(0, tiles)
    def _(j):
        gain = par_ref[5:6, lanes_of(j)]
        for s in range(prompts):
            pre_ref[s, :, lanes_of(j)] = (yacc[s, j] * ssqp[s] * gain).astype(BF16)

    @pl.loop(0, CHIPS)
    def _(k):
        forward_copy(k, lax.rem(q + CHIPS - k, CHIPS), True).wait_recv()

    @pl.loop(1, CTX)
    def _(k):
        square_copy(k, True).wait_recv()

    wcopy.wait()
    squares = ssqr[0]
    for i in range(1, CTX):
        squares = squares + ssqr[i]
    scale = lax.rsqrt(squares * (1.0 / width) + 1e-5)
    scale = jnp.concatenate([scale, jnp.zeros((rows - 8, rows), F32)], 0).T
    pair = 2 * LANES
    flat[...] = dot(gbuf[0], wbuf[:pair, :])

    @pl.loop(1, CHIPS)
    def _(i):
        flat[...] += dot(gbuf[i], wbuf[pl.ds(pl.multiple_of(i * pair, pair), pair), :])

    for i in range(steps):
        fstage[i] = (flat[i * rows : (i + 1) * rows] * scale[:, i : i + 1]).astype(fstage.dtype)
    share = rows // TP

    def rows_of(at):
        return fstage.at[:, pl.ds(pl.multiple_of(at * share, share), share), :]

    def sum_copy(k, source):
        to = lax.rem(t + k, TP)
        at = lax.rem(t + TP - k, TP) if source else t
        return remote(rows_of(to), rbuf.at[at], ts.at[k], tr.at[k], tp=to)

    @pl.loop(1, TP)
    def _(k):
        sum_copy(k, False).start()

    rbuf[t] = fstage[:, pl.ds(pl.multiple_of(t * share, share), share), :]

    rim.wait_send()
    dsend.wait_send()
    forward_copy(0, q, False).wait_send()

    @pl.loop(1, CTX)
    def _(k):
        for copy in decode_copies(k, False):
            copy.wait_send()
        square_copy(k, False).wait_send()

    @pl.loop(0, CHIPS)
    def _(i):
        remote(osend.at[i], orecv.at[i], d2s.at[i], d2r.at[i], ctx=mate).wait_send()
        remote(e2send.at[i], e2recv.at[i], e2s.at[i], e2r.at[i], ctx=mate).wait_send()

    @pl.loop(1, CHIPS)
    def _(k):
        to = chip_at(k) * 2 + core
        remote(ostage.at[q], arecv.at[q], as_.at[k], ar.at[k], ctx=to).wait_send()
        remote(dstage.at[q], dchip.at[q], ads.at[k], adr.at[k], ctx=to).wait_send()
        remote(retst.at[q], erecv.at[q], rs_.at[k], rr.at[k], ctx=to).wait_send()
        gather_copy(k, False).wait_send()
        forward_copy(k, lax.rem(q + CHIPS - k, CHIPS), False).wait_send()

    @pl.loop(1, TP)
    def _(k):
        sum_copy(k, True).wait_recv()

    total = rbuf[0].astype(F32)
    for i in range(1, TP):
        total = total + rbuf[i].astype(F32)
    lay_ref[...] = total.astype(BF16)

    @pl.loop(1, TP)
    def _(k):
        sum_copy(k, False).wait_send()


def shards(
    inner_x, gate_z, proj_bc, dt_raw, a_log, dt_bias, d_skip, conv_x, conv_bc, bias_x, bias_bc,
    norm_gain, init_state, init_conv_x, init_conv_bc, lengths, dec_x, dec_z, dec_bc, dec_dt,
    row_prompt, w_out,
):
    prompts, tokens, width = inner_x.shape
    bc_width = proj_bc.shape[3]
    states = bc_width // 2
    heads = dt_raw.shape[1]
    head = width // heads
    steps, batch = dec_x.shape[:2]
    out_width = w_out.shape[1]
    tiles = width // LANES
    rows = batch * CTX
    rate = jnp.exp(a_log)

    def over(v):
        return jnp.repeat(v, head)[None]

    par = jnp.concatenate(
        [conv_x, bias_x[None], norm_gain[None], over(d_skip), over(rate)], 0
    )
    pbc = jnp.concatenate(
        [conv_bc.reshape(4, bc_width), bias_bc, jnp.zeros((3, bc_width), F32)], 0
    )
    hp = jnp.broadcast_to(jnp.stack([rate, dt_bias])[:, :, None], (2, heads, tokens))
    rim0 = jnp.concatenate([init_conv_x, init_conv_bc.reshape(prompts, 3, bc_width)], -1)
    rim0 = jnp.pad(rim0.astype(F32), ((0, 0), (5, 0), (0, 0))).reshape(8 * prompts, -1)
    stepd = softplus(dec_dt + dt_bias[None, :, None])
    stepd = jnp.transpose(stepd, (2, 0, 1)).reshape(batch, steps * heads)
    which = jnp.broadcast_to(row_prompt[:, None].astype(F32), (batch, LANES))
    small = jnp.stack([stepd, which])

    vm = pl.BlockSpec(memory_space=pltpu.VMEM)
    hb = pl.BlockSpec(memory_space=pltpu.HBM)
    sm = pl.BlockSpec(memory_space=pltpu.SMEM)
    dma = pltpu.SemaphoreType.DMA
    V = pltpu.VMEM
    state = (CHIPS, prompts, states, LANES)
    tile = (prompts, tiles, tokens, LANES)
    scratch = [
        V((prompts, tokens, width), BF16),
        V((prompts, LANES, states), F32),
        V((width, out_width), BF16),
        V((8 * prompts, width + bc_width), BF16),
        V((8 * prompts, width + bc_width), BF16),
        V((8 * prompts, width + bc_width), F32),
        V((8 * prompts, width), BF16),
        V((8 * prompts, bc_width), BF16),
        V((steps, CTX, batch, LANES), BF16),
        V((steps, CTX, batch, LANES), BF16),
        V((steps, CTX, batch, bc_width), BF16),
        V((CTX, 2, batch, LANES), F32),
        V((CTX, 8 * prompts, LANES), BF16),
        V((CTX, 8 * prompts, bc_width), BF16),
        V((prompts, heads, tokens), F32),
        V((prompts, tokens, tokens), F32),
        V((prompts, states, 2 * tokens), BF16),
        V((prompts, 2 * tokens, states), BF16),
        V((prompts, tokens, tokens), F32),
        V((8, width), F32),
        V((8, CHIPS * LANES), F32),
        V((CHIPS, 8, LANES), F32),
        V((CHIPS, 8, LANES), F32),
        V(state, F32),
        V(state, F32),
        V(state, F32),
        V(state, BF16),
        V(state, BF16),
        V((prompts, states, LANES), F32),
        V(state, BF16),
        V(state, BF16),
        V(state, BF16),
        V(state, BF16),
        V(tile, F32),
        V(tile, F32),
        V(tile, F32),
        V((prompts, tokens, LANES), F32),
        V((tiles // 2, steps * rows, 2 * LANES), BF16),
        V((8, rows), F32),
        V((CTX, 8, rows), F32),
        V((steps * rows, out_width), F32),
        V((steps, rows, out_width), F32),
        V((TP, steps, rows // TP, out_width), F32),
        dma((3,)),
        dma,
        dma,
        dma((6, CTX)),
        dma((6, CTX)),
        dma((CHIPS,)),
        dma((CHIPS,)),
        dma,
        dma,
        *[dma((CHIPS,)) for _ in range(12)],
        dma((CTX,)),
        dma((CTX,)),
        dma((TP,)),
        dma((TP,)),
    ]
    return pl.pallas_call(
        kernel,
        out_shape=(
            jax.ShapeDtypeStruct((prompts, tokens, width), BF16),
            jax.ShapeDtypeStruct((steps, rows // TP, out_width), BF16),
        ),
        in_specs=[vm, vm, hb, vm, vm, vm, vm, hb, vm, vm, vm, vm, vm, sm, hb],
        out_specs=(vm, vm),
        scratch_shapes=scratch,
        compiler_params=pltpu.CompilerParams(
            collective_id=0, has_side_effects=True, vmem_limit_bytes=60 * 2**20
        ),
        name="mixer",
    )(
        inner_x, proj_bc.reshape(prompts, tokens, bc_width), gate_z, dt_raw, par, pbc, hp,
        init_state.reshape(prompts, tiles, LANES, states), rim0, dec_x, dec_z,
        dec_bc.reshape(steps, batch, bc_width), small, lengths, w_out,
    )


def solution(mesh):
    ctx, tp = "ctx", "tp"
    placed = (
        P(None, ctx, tp), P(None, ctx, tp), P(None, ctx, tp, None), P(None, tp, ctx),
        P(tp), P(tp), P(tp), P(None, tp), P(None, tp, None), P(tp), P(tp, None), P(tp),
        P(None, tp, None, None), P(None, None, tp), P(None, None, tp, None), P(),
        P(None, ctx, tp), P(None, ctx, tp), P(None, ctx, tp, None), P(None, tp, ctx),
        P(ctx), P(tp, ctx),
    )
    return jax.shard_map(
        shards,
        mesh=mesh,
        in_specs=placed,
        out_specs=(P(None, ctx, tp), P(None, tp, ctx)),
        check_vma=False,
    )
```

```python
import functools

import jax
import jax.numpy as jnp
from jax import lax
from jax.experimental import pallas as pl
from jax.experimental.pallas import tpu as pltpu
from jax.sharding import PartitionSpec as P

MESH = pl.DeviceIdType.MESH
F32, BF16 = jnp.float32, jnp.bfloat16
HIGH = lax.Precision.HIGHEST
LANES = 128
CHIPS, CTX, TP, PAIRS = 8, 16, 8, 4
PARTS = 4
FINISH = (3, 3)


def split(v):
    high = v.astype(BF16)
    return high, (v - high.astype(F32)).astype(BF16)


def dot(a, b):
    return jnp.dot(a, b, preferred_element_type=F32)


def silu(v):
    return v / (1.0 + jnp.exp(-v))


def softplus(v):
    return jnp.maximum(v, 0.0) + jnp.log1p(jnp.exp(-jnp.abs(v)))


def kernel(
    x_hbm, bc_hbm, z_hbm, dt_ref, alog_ref, dtb_ref, dsk_ref, cx_ref, cbc_ref, bx_ref, bbc_ref,
    gain_ref, init_hbm, icx_ref, icbc_ref, len_ref, dx_hbm, dz_hbm, dbc_hbm, ddt_ref, rp_ref, w_hbm,
    pre_hbm, lay_ref,
    x_ref, bc_ref, dx_ref, dz_ref, dbc_ref, pre_ref,
    zbuf, ibuf, wbuf, rimsend, rimrecv, rimf, tailx, tailbc, small, spread4, hrow,
    dxr, dzr, dbcr, smr, txr, tbr,
    runrows, cols, bthl, chl, scs, dall, drecv, ydsend, ydrecv, dchip, zdsend, zdrecv,
    osend, oown, orecv, ysend, yrecv, ochip, zsend, zrecv, est, retst, erecv, yesend, yerecv,
    e2send, e2recv, emine,
    vp, er, yacc, ssqp, gbuf, ssqs, ssqr, flat, fstage, rbuf, lsem, sems,
):
    c, t = lax.axis_index("ctx"), lax.axis_index("tp")
    q, core = lax.div(c, 2), lax.rem(c, 2)
    mate = q * 2 + (1 - core)
    blk = core * CHIPS + q
    prompts, tokens, width = x_ref.shape
    tiles = width // LANES
    states = init_hbm.shape[3]
    steps, batch = dx_ref.shape[:2]
    rows = batch * CTX
    heads = dt_ref.shape[1]

    barrier = pltpu.get_barrier_semaphore()
    for k in range(1, CTX):
        pl.semaphore_signal(barrier, inc=1, device_id=(lax.rem(c + k, CTX), t), device_id_type=MESH)
    for k in range(1, TP):
        pl.semaphore_signal(barrier, inc=1, device_id=(c, lax.rem(t + k, TP)), device_id_type=MESH)

    def lanes_of(j, size=LANES):
        return pl.ds(pl.multiple_of(j * size, size), size)

    def remote(src, dst, ssem, rsem, ctx=None, tp=None):
        return pltpu.make_async_remote_copy(
            src_ref=src, dst_ref=dst, send_sem=ssem, recv_sem=rsem,
            device_id=(c if ctx is None else ctx, t if tp is None else tp),
            device_id_type=MESH,
        )

    zed, why = lax.div(q, 2), lax.rem(q, 2)
    neighbour = (2 * zed + 1 - why) * 2 + core

    def device_of(chip):
        return chip * 2 + core

    def zed_at(k):
        return lax.rem(zed + k, PAIRS)

    def zed_from(k):
        return lax.rem(zed + PAIRS - k, PAIRS)

    taken = []

    def new(count=None):
        base = sum(taken)
        taken.append(count or 1)
        return sems.at[base] if count is None else lambda k: sems.at[base + k]

    def wait_sent(sem, ref):
        remote(ref, ref, sem, sem, ctx=mate).wait_send()

    def wait_got(sem, ref):
        remote(ref, ref, sem, sem, ctx=mate).wait_recv()

    rims, rimr = new(), new()
    decs, decr = new(3), new(3)
    sps, spn, spr, psr = new(3), new(3), new(3), new(3)
    d2s, d2r, dds, ddr, e2s, e2r = new(), new(CHIPS), new(), new(), new(), new()
    yos, yor, yds, ydr = new(), new(PAIRS), new(), new()
    zos, zor, zds, zdr = new(), new(PAIRS), new(), new()
    rs_, rr, yes_, yer = new(), new(PAIRS), new(), new(PAIRS)
    gns, gqs, gfs = new(), new(), new()
    gnr, gzr, gqr, gfr, qr, tr = [new(PARTS) for _ in range(6)]
    qs, ts = new(), new()
    assert sum(taken) == sems.shape[0]

    def load(at, src, dst):
        copy = pltpu.make_async_copy(src, dst, lsem.at[at])
        copy.start()
        return copy

    xcopy, bcopy = load(0, x_hbm, x_ref), load(1, bc_hbm, bc_ref)
    dcopies = [
        load(2, dx_hbm, dx_ref), load(3, dz_hbm, dz_ref), load(4, dbc_hbm, dbc_ref)
    ]
    icopy = load(5, init_hbm.at[:, blk], ibuf)
    zcopy, wcopy = load(6, z_hbm, zbuf), load(7, w_hbm, wbuf)

    hrow[...] = jnp.zeros_like(hrow)
    hrow[0:1, :heads] = jnp.exp(alog_ref[...])
    hrow[1:2, :heads] = dtb_ref[...]
    hrow[2:3, :heads] = dsk_ref[...]
    spread4[...] = jnp.zeros_like(spread4)
    for i in range(steps):
        spread4[i, :, :heads] = softplus(ddt_ref[i] + hrow[1:2, :heads])
    small[0] = sum(
        spread4[i] if i == 0 else pltpu.roll(spread4[i], heads * i, 1) for i in range(steps)
    )
    which = jnp.zeros((batch, LANES), F32)
    row_at = lax.broadcasted_iota(jnp.int32, (batch, LANES), 0)
    for r in range(batch):
        which = jnp.where(row_at == r, rp_ref[r].astype(F32), which)
    small[1] = which

    upto = lax.broadcasted_iota(jnp.int32, (tokens, tokens), 0)
    at_lane = lax.broadcasted_iota(jnp.int32, (tokens, tokens), 1)
    upper = jnp.where(upto <= at_lane, 1.0, 0.0)
    lower = upto >= at_lane
    hcol = jnp.concatenate([hrow[...], jnp.zeros((LANES - 8, LANES), F32)], 0).T
    rate_col, bias_col = hcol[:heads, 0:1], hcol[:heads, 1:2]
    lane_place = lax.broadcasted_iota(jnp.int32, (heads, tokens), 1) + c * tokens
    for s in range(prompts):
        live = lane_place < len_ref[s]
        step = jnp.where(live, softplus(dt_ref[s] + bias_col), 0.0)
        run = jnp.dot(-rate_col * step, upper, precision=HIGH, preferred_element_type=F32)
        runrows[s] = run
        both = jnp.concatenate([run, step, jnp.zeros((tokens - 2 * heads, tokens), F32)], 0)
        cols[s] = both.T
    first_half = lax.broadcasted_iota(jnp.int32, (tokens, LANES), 1) < LANES // 2
    ends = [cols[s][tokens - 1 :] for s in range(prompts)]
    ends = jnp.exp(jnp.concatenate(ends + [jnp.zeros((8 - prompts, LANES), F32)], 0))
    for j in range(tiles):
        dall[j] = jnp.where(first_half[:8], ends[:, 2 * j : 2 * j + 1], ends[:, 2 * j + 1 : 2 * j + 2])

    xcopy.wait()
    bcopy.wait()
    ends = [x_ref[s, tokens - 16 :, :].astype(F32)[8:] for s in range(prompts)]
    rimsend[:, :width] = jnp.concatenate(ends, 0).astype(BF16)
    ends = [bc_ref[s, tokens - 16 :, :].astype(F32)[8:] for s in range(prompts)]
    rimsend[:, width:] = jnp.concatenate(ends, 0).astype(BF16)
    pl.semaphore_wait(barrier, CTX - 1 + TP - 1)

    rim = remote(rimsend, rimrecv, rims, rimr, ctx=lax.rem(c + 1, CTX))
    pl.when(c != CTX - 1)(rim.start)
    half = pl.ds(pl.multiple_of((1 - core) * CHIPS, CHIPS), CHIPS)
    remote(dall.at[half], drecv, dds, ddr, ctx=mate).start()

    place = lax.broadcasted_iota(jnp.int32, (8, tokens), 1) + c * tokens
    slot = lax.broadcasted_iota(jnp.int32, (8, tokens), 0)
    tx, tbc = 0.0, 0.0
    for s in range(prompts):
        hit = (place == len_ref[s] - 3 + slot - 4 * s) & (slot >= 4 * s) & (slot < 4 * s + 3)
        pick = jnp.where(hit, 1.0, 0.0).astype(BF16)
        tx = tx + dot(pick, x_ref[s])
        tbc = tbc + dot(pick, bc_ref[s])
    tailx[...] = tx.astype(BF16)
    tailbc[...] = tbc.astype(BF16)

    for copy in dcopies:
        copy.wait()
    dxr[:, c] = dx_ref[:, :, lanes_of(blk)]
    dzr[:, c] = dz_ref[:, :, lanes_of(blk)]
    dbcr[:, c] = dbc_ref[...]
    smr[c] = small[...]
    txr[c] = tailx[:, lanes_of(blk)]
    tbr[c] = tailbc[...]

    def scatter_copies(k, source):
        to = lax.rem(c + k, CTX)
        their = lax.rem(to, 2) * CHIPS + lax.div(to, 2)
        at = lax.rem(c + CTX - k, CTX) if source else c
        pairs = (
            (dx_ref.at[:, :, lanes_of(their)], dxr.at[:, at]),
            (dz_ref.at[:, :, lanes_of(their)], dzr.at[:, at]),
            (tailx.at[:, lanes_of(their)], txr.at[at]),
        )
        return [
            remote(src, dst, decs(i), decr(i), ctx=to)
            for i, (src, dst) in enumerate(pairs)
        ]

    spread_refs = (dbc_ref, small, tailbc)

    def spread_to(at):
        return dbcr.at[:, at], smr.at[at], tbr.at[at]

    def spread_copies(k, source):
        if isinstance(k, int):
            to, at = neighbour, neighbour
        else:
            to, at = device_of(2 * zed_at(k) + why), device_of(2 * zed_from(k) + why)
        return [
            remote(src, dst, sps(i), spn(i) if isinstance(k, int) else spr(i), ctx=to)
            for i, (src, dst) in enumerate(zip(spread_refs, spread_to(at if source else c)))
        ]

    def relay_copies(k, source):
        at = device_of(2 * (zed_from(k) if source else zed) + 1 - why)
        return [
            remote(ref, ref, sps(i), spr(i), ctx=device_of(2 * zed_at(k) + why))
            for i, ref in enumerate(spread_to(at))
        ]

    def pass_copies(chip, source):
        at = chip * 2 + (1 - core if source else core)
        return [
            remote(ref, ref, sps(i), psr(i), ctx=mate)
            for i, ref in enumerate(spread_to(at))
        ]

    @pl.loop(1, CTX)
    def _(k):
        for copy in scatter_copies(k, False):
            copy.start()

    for copy in spread_copies(0, False):
        copy.start()

    @pl.loop(1, PAIRS)
    def _(k):
        for copy in spread_copies(k, False):
            copy.start()

    def entry_copy(k, source):
        to = zed_at(k)
        src, at = (zed, zed_from(k)) if source else (to, zed)
        return remote(
            retst.at[src], erecv.at[at], rs_, rr(k), ctx=device_of(2 * to + why)
        )

    icopy.wait()
    for s in range(prompts):
        est[s] = ibuf[s].T
        retst[0, s] = est[s].astype(BF16)

    @pl.when(zed != 0)
    def _():
        entry_copy(PAIRS - zed, False).start()

    @pl.when(c != 0)
    def _():
        rim.wait_recv()
        rimf[...] = rimrecv[...].astype(F32)

    @pl.when(c == 0)
    def _():
        rimf[...] = jnp.zeros_like(rimf)
        for s in range(prompts):
            for k in range(3):
                at = 8 * s + 5 + k
                rimf[at : at + 1, :width] = icx_ref[k].astype(F32)[s : s + 1]
                rimf[at : at + 1, width:] = icbc_ref[k].astype(F32)[s : s + 1]

    def conv(rim_rows, body, taps, bias):
        padded = jnp.concatenate([rim_rows, body], 0)
        total = bias
        for k in range(4):
            total = total + taps[k] * padded[5 + k : 5 + k + body.shape[0]]
        return silu(total)

    bc_taps = [cbc_ref[k] for k in range(4)]
    for s in range(prompts):
        act = conv(rimf[8 * s : 8 * s + 8, width:], bc_ref[s].astype(F32), bc_taps, bbc_ref[...])
        b, cc = act[:, :states], act[:, states:]
        bt = b.T
        high, low = split(bt)
        bthl[s] = jnp.concatenate([high, low], 1)
        chl[s] = jnp.concatenate(split(cc), 0)
        scores = jnp.dot(cc, bt, precision=HIGH, preferred_element_type=F32)
        scs[s] = jnp.where(lower, scores, 0.0)

    def columns(s, j):
        return pltpu.roll(cols[s], lax.rem(tokens - 2 * j, tokens), 1)

    def per_lane(row, j):
        rolled = pltpu.roll(hrow[...], lax.rem(LANES - 2 * j, LANES), 1)[row : row + 1]
        return jnp.where(first_half[:1], rolled[:, 0:1], rolled[:, 1:2])

    def taps_of(lanes):
        taps = cx_ref[:, lanes]
        return [taps[k : k + 1] for k in range(4)]

    def own_part(j, i, out):
        lanes = lanes_of(j)
        taps, skip = taps_of(lanes), per_lane(2, j)
        for s in range(prompts):
            body = x_ref[s, :, lanes].astype(F32)
            xv = conv(rimf[8 * s : 8 * s + 8, lanes], body, taps, bx_ref[:, lanes])
            col = columns(s, j)
            r = jnp.where(first_half, col[:, 0:1], col[:, 1:2])
            step = jnp.where(first_half, col[:, heads : heads + 1], col[:, heads + 1 : heads + 2])
            end = r[tokens - 1 : tokens]
            v = xv * step
            vp[s, j] = v
            er[s, j] = jnp.exp(r)
            yacc[s, j] = skip * xv
            high, low = split(v * jnp.exp(end - r))
            out[i, s] = dot(bthl[s], jnp.concatenate([high, high], 0)) + dot(
                bthl[s, :, :tokens], low
            )

    is_first = core == 0

    def state_copy(i):
        return remote(osend.at[i], orecv.at[i], d2s, d2r(i), ctx=mate)

    def decays(s, i):
        return dall[core * CHIPS + i, s : s + 1], drecv[i, s : s + 1]

    def pair_copy(at):
        return remote(ysend.at[at], yrecv.at[at], yos, yor(at), ctx=neighbour)

    def zed_copy(k, source, refs, ssem, rsem):
        to = zed_at(k)
        src, at = (zed, zed_from(k)) if source else (to, zed)
        return remote(refs[0].at[src], refs[1].at[at], ssem, rsem, ctx=device_of(2 * to + why))

    def zed_state(k, source):
        return zed_copy(k, source, (zsend, zrecv), zos, zor(k))

    def zed_decay(k):
        return zed_copy(k, False, (zdsend, zdrecv), zds, zdr)

    def block_of(n):
        at = lax.rem(zed + n, PAIRS)
        return at, 2 * at + jnp.where(n <= PAIRS, 1 - why, why)

    is_low = why == 0

    def combine(n):
        at, i = block_of(n)
        state_copy(i).wait_recv()
        for s in range(prompts):
            down, theirs = decays(s, i)
            a = jnp.where(is_first, theirs, 1.0)
            b = jnp.where(is_first, 1.0, down)
            ochip[at, s] = a * oown[i, s] + b * orecv[i, s]

        @pl.when(n <= PAIRS)
        def _():
            for s in range(prompts):
                ysend[at, s] = ochip[at, s].astype(BF16)
            pair_copy(at).start()

    def quad(m):
        at = zed_at(m)
        pair_copy(at).wait_recv()
        for s in range(prompts):
            down, theirs = dchip[at, s : s + 1], ydrecv[at, s : s + 1]
            a = jnp.where(is_low, theirs, 1.0)
            b = jnp.where(is_low, 1.0, down)
            zsend[at, s] = a * ochip[at, s] + b * yrecv[at, s].astype(F32)

    def quad_send(m):
        quad(m)
        zed_state(m, False).start()

    wait_got(ddr, drecv)
    for at in range(PAIRS):
        for ref, i in ((dchip, 2 * at + why), (ydsend, 2 * at + 1 - why)):
            ref[at] = dall[core * CHIPS + i] * drecv[i]
    pair_decays = remote(ydsend, ydrecv, yds, ydr, ctx=neighbour)
    pair_decays.start()

    @pl.loop(1, CHIPS + 1)
    def _(n):
        i = block_of(n)[1]
        own_part((1 - core) * CHIPS + i, i, osend)
        own_part(core * CHIPS + i, i, oown)
        state_copy(i).start()

        @pl.when(n > 1)
        def _():
            combine(n - 1)

        @pl.when(n == 3)
        def _():
            for copy in spread_copies(0, True):
                copy.wait_recv()

            @pl.loop(1, PAIRS)
            def _(k):
                for copy in relay_copies(k, False):
                    copy.start()

            pair_decays.wait_recv()
            zdsend[...] = dchip[...] * ydrecv[...]

            @pl.loop(1, PAIRS)
            def _(k):
                zed_decay(k).start()

        @pl.when(n > PAIRS + 2)
        def _():
            quad_send(n - PAIRS - 2)

    combine(CHIPS)

    def inside(j):
        for s in range(prompts):
            col = columns(s, j)
            mixing = []
            for h in range(2):
                row = runrows[s, pl.ds(2 * j + h, 1), :]
                gap = jnp.minimum(col[:, h : h + 1] - row, 0.0)
                mixing.append((jnp.exp(gap) * scs[s]).astype(BF16))
            both = jnp.concatenate(mixing, 1)
            v = vp[s, j]
            total = yacc[s, j]
            stacked = jnp.concatenate([jnp.where(first_half, v, 0.0), jnp.where(first_half, 0.0, v)], 0)
            for part in split(stacked):
                total = total + dot(both, part)
            yacc[s, j] = total

    cuts = (0, 4, 8, 10)
    pl.loop(0, cuts[1])(inside)
    quad_send(PAIRS - 1)
    pl.loop(cuts[1], cuts[2])(inside)
    quad(PAIRS)
    zrecv[zed] = zsend[zed]
    zdrecv[zed] = zdsend[zed]

    for copy in pass_copies(q, False):
        copy.start()

    for i, ref in enumerate(spread_to(pl.ds(0, 2 * (PAIRS - 1)))):
        wait_got(spr(i), ref)

    @pl.loop(0, CHIPS)
    def _(chip):
        @pl.when(chip != q)
        def _():
            for copy in pass_copies(chip, False):
                copy.start()

    wait_got(zdr, zdrecv.at[: PAIRS - 1])

    @pl.loop(0, PAIRS)
    def _(p):
        @pl.when(p > 0)
        def _():
            for s in range(prompts):
                retst[p, s] = est[s].astype(BF16)

        @pl.when((p > 0) & (p != zed))
        def _():
            entry_copy(lax.rem(p - zed + PAIRS, PAIRS), False).start()

        @pl.when(p != zed)
        def _():
            zed_state(lax.rem(zed - p + PAIRS, PAIRS), True).wait_recv()

        for s in range(prompts):
            est[s] = zdrecv[p, s : s + 1] * est[s] + zrecv[p, s]

    erecv[zed] = retst[zed]

    def entry_to_neighbour(at):
        return remote(yesend.at[at], yerecv.at[at], yes_, yer(at), ctx=neighbour)

    def mate_copy(i):
        return remote(e2send.at[i], e2recv.at[i], e2s, e2r, ctx=mate)

    def for_cores(i, s, e):
        down, theirs = decays(s, i)
        e2send[i, s] = jnp.where(is_first, down * e + oown[i, s], e)
        emine[i, s] = jnp.where(is_first, e, theirs * e + orecv[i, s])

    def entry_step(at):
        i = 2 * at + why
        entries = []
        for s in range(prompts):
            down, theirs = dchip[at, s : s + 1], ydrecv[at, s : s + 1]
            e = erecv[at, s].astype(F32)
            yesend[at, s] = jnp.where(is_low, down * e + ochip[at, s], e).astype(BF16)
            entries.append(jnp.where(is_low, e, theirs * e + yrecv[at, s].astype(F32)))
        entry_to_neighbour(at).start()
        for s in range(prompts):
            for_cores(i, s, entries[s])
        mate_copy(i).start()

    entry_step(zed)

    others = (dxr.at[:, : CTX - 1], dzr.at[:, : CTX - 1], txr.at[: CTX - 1])
    for i, ref in enumerate(others):
        wait_got(decr(i), ref)
    for i, ref in enumerate(spread_to(pl.ds(0, CHIPS))):
        wait_got(psr(i), ref)

    part_steps = steps // PARTS
    part = part_steps * rows

    def slab(chip, which, h):
        at = which * CHIPS + chip
        return gbuf.at[lax.div(at, 2), h * part : (h + 1) * part, lanes_of(lax.rem(at, 2))]

    def to_neighbour(h, source):
        at = 2 * zed + (1 - why if source else why)
        return remote(slab(q, core, h), slab(at, core, h), gns, gnr(h), ctx=neighbour)

    def gather_copy(k, h, source):
        at = 2 * zed_from(k) + why if source else q
        to = device_of(2 * zed_at(k) + why)
        return remote(slab(q, core, h), slab(at, core, h), gns, gzr(h), ctx=to)

    def relay_copy(k, h, source):
        piece = slab(2 * (zed_from(k) if source else zed) + 1 - why, core, h)
        to = device_of(2 * zed_at(k) + why)
        return remote(piece, piece, gqs, gqr(h), ctx=to)

    def forward_copy(chip, h, source):
        piece = slab(chip, 1 - core if source else core, h)
        return remote(piece, piece, gfs, gfr(h), ctx=mate)

    def square_copy(k, h, source):
        at = lax.rem(c + CTX - k, CTX) if source else c
        to = lax.rem(c + k, CTX)
        return remote(ssqs.at[h], ssqr.at[h, at], qs, qr(h), ctx=to)

    def send_along(h):
        @pl.loop(1, PAIRS)
        def _(k):
            gather_copy(k, h, False).start()

    def send_rows(h):
        to_neighbour(h, False).start()
        if h == 0:
            send_along(h)
        forward_copy(q, h, False).start()

        @pl.loop(1, CTX)
        def _(k):
            square_copy(k, h, False).start()

    def relay_rows(h):
        to_neighbour(h, True).wait_recv()

        @pl.loop(1, PAIRS)
        def _(k):
            relay_copy(k, h, False).start()

        if h + 1 < PARTS:
            send_along(h + 1)
        forward_copy(2 * zed + 1 - why, h, False).start()

    lanes = lanes_of(blk)
    taps, bias, gain = taps_of(lanes), bx_ref[:, lanes], gain_ref[:, lanes]
    rate, skip = per_lane(0, blk), per_lane(2, blk)
    second = smr[:, 1].reshape(rows, LANES)[:, 0:1] > 0.5
    sizes = smr[:, 0].reshape(rows, LANES)
    rolled = pltpu.roll(sizes, lax.rem(LANES - 2 * blk, LANES), 1)

    def window(ref):
        out = ref[0].astype(F32)
        for i in range(1, CTX):
            out = out + ref[i].astype(F32)
        return [jnp.where(second, out[4 + k : 5 + k], out[k : k + 1]) for k in range(3)]

    def flat_rows(ref, i):
        return ref[i].astype(F32).reshape(rows, ref.shape[3])

    seq_x = window(txr) + [flat_rows(dxr, i) for i in range(steps)]
    seq_b = window(tbr) + [flat_rows(dbcr, i) for i in range(steps)]

    def taps_on(seq, i, weights, total):
        for k in range(4):
            total = total + weights[k] * seq[i + k]
        return silu(total)

    final = [split(est[s]) for s in range(prompts)]
    bs, us = [], []
    grown = 1.0
    row8 = lax.broadcasted_iota(jnp.int32, (8, LANES), 0)
    for i in range(steps):
        xd = taps_on(seq_x, i, taps, bias)
        bcd = taps_on(seq_b, i, bc_taps, bbc_ref[...])
        cd = bcd[:, states:]
        chigh, clow = split(cd)
        at = heads * i
        step = jnp.where(first_half, rolled[:, at : at + 1], rolled[:, at + 1 : at + 2])
        keep = jnp.exp(-rate * step)
        grown = grown * keep
        bs.append(bcd[:, :states])
        us = [keep * u for u in us] + [step * xd]
        y0 = [
            dot(chigh, high) + dot(clow, high) + dot(chigh, low) for high, low in final
        ]
        yd = grown * jnp.where(second, y0[1], y0[0]) + skip * xd
        for b, u in zip(bs, us):
            yd = yd + u * jnp.sum(b * cd, axis=1, keepdims=True)
        m = yd * silu(flat_rows(dzr, i))
        if i % part_steps == 0:
            squares = jnp.zeros((8, rows), F32)
        squares = squares + lax.dot_general(
            jnp.where(row8 == i, 1.0, 0.0), m * m, (((1,), (1,)), ((), ())),
            precision=HIGH, preferred_element_type=F32,
        )
        gbuf[lax.div(blk, 2), i * rows : (i + 1) * rows, lanes_of(lax.rem(blk, 2))] = (
            m * gain
        ).astype(BF16)
        if i % part_steps == part_steps - 1:
            ssqs[i // part_steps] = squares
            ssqr[i // part_steps, c] = squares
            send_rows(i // part_steps)

    pl.loop(cuts[2], cuts[3])(inside)
    for h in range(PARTS):
        relay_rows(h)
        if h + 1 < PAIRS:
            entry_copy(h + 1, True).wait_recv()
            entry_step(zed_from(h + 1))
            pl.loop(cuts[3] + 2 * h, cuts[3] + 2 * h + 2)(inside)

    zcopy.wait()
    ssqp[...] = jnp.zeros_like(ssqp)

    def finish(s, j, entry):
        high, low = split(entry)
        carried = dot(chl[s], high)
        carried = carried[:tokens] + carried[tokens:] + dot(chl[s, :tokens], low)
        y = yacc[s, j] + carried * er[s, j]
        m = y * silu(zbuf[s, :, lanes_of(j)].astype(F32))
        yacc[s, j] = m
        ssqp[s] += m * m

    def finish_mine(i):
        for s in range(prompts):
            finish(s, core * CHIPS + i, emine[i, s])

    def own_column():
        @pl.loop(0, PAIRS)
        def _(k):
            finish_mine(2 * zed_from(k) + why)

    def other_column():
        @pl.loop(0, PAIRS)
        def _(k):
            at = zed_from(k)
            i = 2 * at + 1 - why
            entry_to_neighbour(at).wait_recv()
            for s in range(prompts):
                for_cores(i, s, yerecv[at, s].astype(F32))
            mate_copy(i).start()
            finish_mine(i)

    def other_core():
        wait_got(e2r, e2recv)

        @pl.loop(0, CHIPS)
        def _(i):
            for s in range(prompts):
                finish(s, (1 - core) * CHIPS + i, e2recv[i, s])

    wcopy.wait()
    pair, groups = 2 * LANES, CHIPS // 2
    share = rows // TP

    def projected(which, h):
        total = 0.0
        for g in range(groups):
            at = which * groups + g
            w = wbuf[pl.ds(pl.multiple_of(at * pair, pair), pair), :]
            total = total + dot(gbuf[at, h * part : (h + 1) * part], w)
        return total

    def rows_of(at):
        return pl.ds(pl.multiple_of(at * share, share), share)

    def sum_copy(k, h, source):
        to = lax.rem(t + k, TP)
        at = lax.rem(t + TP - k, TP) if source else t
        these = slice(h * part_steps, (h + 1) * part_steps)
        return remote(
            fstage.at[these, rows_of(to), :], rbuf.at[at, these], ts, tr(h), tp=to
        )

    for h in range(PARTS):

        three = gbuf.at[0, : (PAIRS - 1) * part // 2]
        wait_got(gzr(h), three)

        @pl.loop(1, PAIRS)
        def _(k):
            forward_copy(2 * zed_from(k) + why, h, False).start()

        wait_got(gqr(h), three)

        @pl.loop(1, PAIRS)
        def _(k):
            forward_copy(2 * zed_from(k) + 1 - why, h, False).start()

        flat[...] = projected(core, h)

        if h == 0:
            own_column()
        wait_got(gfr(h), gbuf.at[0])
        wait_got(qr(h), ssqr.at[h, : CTX - 1])

        squares = ssqr[h, 0]
        for i in range(1, CTX):
            squares = squares + ssqr[h, i]
        scale = lax.rsqrt(squares * (1.0 / width) + 1e-5)
        scale = jnp.concatenate([scale, jnp.zeros((rows - 8, rows), F32)], 0).T
        total = flat[...] + projected(1 - core, h)
        for i in range(part_steps):
            at = h * part_steps + i
            fstage[at] = (total[i * rows : (i + 1) * rows] * scale[:, at : at + 1]).astype(BF16)

        @pl.loop(1, TP)
        def _(k):
            sum_copy(k, h, False).start()

        if h == FINISH[0]:
            other_column()
        if h == FINISH[1]:
            other_core()

    rbuf[t] = fstage[:, rows_of(t), :]

    for s in range(prompts):
        mean = jnp.sum(ssqp[s], axis=1, keepdims=True) * (1.0 / width)
        ssqp[s] = jnp.broadcast_to(lax.rsqrt(mean + 1e-5), ssqp.shape[1:])

    outs = []
    for s in range(prompts):

        @pl.loop(0, tiles)
        def _(j):
            gain = gain_ref[:, lanes_of(j)]
            pre_ref[s, :, lanes_of(j)] = (yacc[s, j] * ssqp[s] * gain).astype(BF16)

        outs.append(pltpu.make_async_copy(pre_ref.at[s], pre_hbm.at[s], lsem.at[s]))
        outs[s].start()

    pl.when(c != CTX - 1)(rim.wait_send)
    wait_sent(dds, drecv)

    for i, ref in enumerate(others):
        wait_sent(decs(i), ref)
    for i, ref in enumerate(spread_to(pl.ds(0, CTX - 1))):
        wait_sent(sps(i), ref)
    three = slice(0, PAIRS - 1)
    for sem, ref in (
        (d2s, osend), (e2s, e2send), (yos, ysend), (yds, ydsend), (yes_, yesend),
        (zos, zsend.at[three]), (zds, zdsend.at[three]), (rs_, retst.at[three]),
        (gns, gbuf.at[:2]), (gqs, gbuf.at[three, : steps * rows // 2]), (gfs, gbuf.at[:4]),
        (qs, ssqr.at[:, : CTX - 1]),
    ):
        wait_sent(sem, ref)

    for h in range(PARTS):
        wait_got(tr(h), rbuf.at[: TP - 1, h * part_steps : (h + 1) * part_steps])

    total = rbuf[0].astype(F32)
    for i in range(1, TP):
        total = total + rbuf[i].astype(F32)
    lay_ref[...] = total.astype(BF16)

    wait_sent(ts, rbuf.at[: TP - 1])

    for copy in outs:
        copy.wait()


def hand_on(a_hbm, b_hbm, a_out, b_out, abuf, bbuf, isem, osem):
    pieces = [(b_hbm, bbuf, b_out)]
    half = a_hbm.shape[1] // 2
    for s in range(a_hbm.shape[0]):
        for r in range(2):
            at = (s, slice(r * half, (r + 1) * half))
            pieces.append((a_hbm.at[at], abuf.at[at], a_out.at[at]))
    into = [pltpu.make_async_copy(a, b, isem.at[i]) for i, (a, b, _) in enumerate(pieces)]
    out = [pltpu.make_async_copy(b, o, osem.at[i]) for i, (_, b, o) in enumerate(pieces)]
    for copy in into:
        copy.start()
    for first, then in zip(into, out):
        first.wait()
        then.start()
    for copy in out:
        copy.wait()


def shards(
    inner_x, gate_z, proj_bc, dt_raw, a_log, dt_bias, d_skip, conv_x, conv_bc, bias_x, bias_bc,
    norm_gain, init_state, init_conv_x, init_conv_bc, lengths, dec_x, dec_z, dec_bc, dec_dt,
    row_prompt, w_out,
):
    prompts, tokens, width = inner_x.shape
    bc_width = proj_bc.shape[3]
    states = bc_width // 2
    heads = dt_raw.shape[1]
    steps, batch = dec_x.shape[:2]
    out_width = w_out.shape[1]
    tiles = width // LANES
    rows = batch * CTX
    vm = pl.BlockSpec(memory_space=pltpu.VMEM)
    hb = pl.BlockSpec(memory_space=pltpu.HBM)
    sm = pl.BlockSpec(memory_space=pltpu.SMEM)
    dma = pltpu.SemaphoreType.DMA
    V = pltpu.VMEM
    state = (CHIPS, prompts, states, LANES)
    pairs = (PAIRS, prompts, states, LANES)
    tile = (prompts, tiles, tokens, LANES)
    scratch = [
        V((prompts, tokens, width), BF16),
        V((prompts, tokens, bc_width), BF16),
        V((steps, batch, width), BF16),
        V((steps, batch, width), BF16),
        V((steps, batch, bc_width), BF16),
        V((prompts, tokens, width), BF16),
        V((prompts, tokens, width), BF16),
        V((prompts, LANES, states), F32),
        V((width, out_width), BF16),
        V((8 * prompts, width + bc_width), BF16),
        V((8 * prompts, width + bc_width), BF16),
        V((8 * prompts, width + bc_width), F32),
        V((8, width), BF16),
        V((8, bc_width), BF16),
        V((2, batch, LANES), F32),
        V((steps, batch, LANES), F32),
        V((8, LANES), F32),
        V((steps, CTX, batch, LANES), BF16),
        V((steps, CTX, batch, LANES), BF16),
        V((steps, CTX, batch, bc_width), BF16),
        V((CTX, 2, batch, LANES), F32),
        V((CTX, 8, LANES), BF16),
        V((CTX, 8, bc_width), BF16),
        V((prompts, heads, tokens), F32),
        V((prompts, tokens, tokens), F32),
        V((prompts, states, 2 * tokens), BF16),
        V((prompts, 2 * tokens, states), BF16),
        V((prompts, tokens, tokens), F32),
        V((tiles, 8, LANES), F32),
        V((CHIPS, 8, LANES), F32),
        *[V((PAIRS, 8, LANES), F32) for _ in range(5)],
        V(state, F32),
        V(state, F32),
        V(state, F32),
        V(pairs, BF16),
        V(pairs, BF16),
        V(pairs, F32),
        V(pairs, F32),
        V(pairs, F32),
        V((prompts, states, LANES), F32),
        V(pairs, BF16),
        V(pairs, BF16),
        V(pairs, BF16),
        V(pairs, BF16),
        V(state, F32),
        V(state, F32),
        V(state, F32),
        V(tile, F32),
        V(tile, F32),
        V(tile, F32),
        V((prompts, tokens, LANES), F32),
        V((tiles // 2, steps * rows, 2 * LANES), BF16),
        V((PARTS, 8, rows), F32),
        V((PARTS, CTX, 8, rows), F32),
        V((steps * rows // PARTS, out_width), F32),
        V((steps, rows, out_width), BF16),
        V((TP, steps, rows // TP, out_width), BF16),
        dma((8,)),
        dma((86,)),
    ]
    prefill, layer = pl.pallas_call(
        kernel,
        out_shape=(
            jax.ShapeDtypeStruct((prompts, tokens, width), BF16),
            jax.ShapeDtypeStruct((steps, rows // TP, out_width), BF16),
        ),
        in_specs=[hb, hb, hb, *[vm] * 9, hb, vm, vm, sm, hb, hb, hb, vm, sm, hb],
        out_specs=(hb, vm),
        scratch_shapes=scratch,
        compiler_params=pltpu.CompilerParams(
            collective_id=0, has_side_effects=True, vmem_limit_bytes=60 * 2**20
        ),
        name="mixer",
    )(
        inner_x, proj_bc.reshape(prompts, tokens, bc_width), gate_z, dt_raw,
        a_log[None], dt_bias[None], d_skip[None], conv_x, conv_bc, bias_x[None], bias_bc,
        norm_gain[None], init_state.reshape(prompts, tiles, LANES, states),
        jnp.transpose(init_conv_x, (1, 0, 2)),
        jnp.transpose(init_conv_bc, (1, 2, 0, 3)).reshape(3, prompts, bc_width),
        lengths, dec_x, dec_z, dec_bc.reshape(steps, batch, bc_width),
        jnp.transpose(dec_dt, (0, 2, 1)), row_prompt, w_out,
    )
    halves = (prompts, tokens, width), (steps, rows // TP, out_width)
    return pl.pallas_call(
        hand_on,
        out_shape=tuple(jax.ShapeDtypeStruct(shape, BF16) for shape in halves),
        in_specs=[hb, hb],
        out_specs=(hb, hb),
        scratch_shapes=[*[V(shape, BF16) for shape in halves], dma((5,)), dma((5,))],
        name="results",
    )(prefill, layer)


def solution(mesh):
    ctx, tp = "ctx", "tp"
    placed = (
        P(None, ctx, tp), P(None, ctx, tp), P(None, ctx, tp, None), P(None, tp, ctx),
        P(tp), P(tp), P(tp), P(None, tp), P(None, tp, None), P(tp), P(tp, None), P(tp),
        P(None, tp, None, None), P(None, None, tp), P(None, None, tp, None), P(),
        P(None, ctx, tp), P(None, ctx, tp), P(None, ctx, tp, None), P(None, tp, ctx),
        P(ctx), P(tp, ctx),
    )
    return jax.shard_map(
        shards,
        mesh=mesh,
        in_specs=placed,
        out_specs=(P(None, ctx, tp), P(None, tp, ctx)),
        check_vma=False,
    )
```

```python
import functools

import jax
import jax.numpy as jnp
from jax import lax
from jax.experimental import pallas as pl
from jax.experimental.pallas import tpu as pltpu
from jax.sharding import PartitionSpec as P

MESH = pl.DeviceIdType.MESH
F32, BF16 = jnp.float32, jnp.bfloat16
HIGH = lax.Precision.HIGHEST
LANES = 128
CHIPS, CTX, TP, PAIRS = 8, 16, 8, 4
PARTS = 4
FINISH = (3, 3)


def split(v):
    high = v.astype(BF16)
    return high, (v - high.astype(F32)).astype(BF16)


def dot(a, b):
    return jnp.dot(a, b, preferred_element_type=F32)


def silu(v):
    return v / (1.0 + jnp.exp(-v))


def softplus(v):
    return jnp.maximum(v, 0.0) + jnp.log1p(jnp.exp(-jnp.abs(v)))


def kernel(
    x_hbm, bc_hbm, z_hbm, dt_ref, alog_ref, dtb_ref, dsk_ref, cx_ref, cbc_ref, bx_ref, bbc_ref,
    gain_ref, init_hbm, icx_ref, icbc_ref, len_ref, dx_hbm, dz_hbm, dbc_hbm, ddt_ref, rp_ref, w_hbm,
    pre_hbm, lay_ref,
    x_ref, bc_ref, dx_ref, dz_ref, dbc_ref, pre_ref,
    zbuf, ibuf, wbuf, rimsend, rimrecv, rimf, tailx, tailbc, small, spread4, hrow,
    dxr, dzr, dbcr, smr, txr, tbr,
    runrows, cols, bthl, chl, scs, dall, drecv, ydsend, ydrecv, dchip, zdsend, zdrecv,
    osend, oown, orecv, ysend, yrecv, ochip, zsend, zrecv, est, retst, erecv, yesend, yerecv,
    e2send, e2recv, emine,
    vp, er, yacc, ssqp, gbuf, ssqs, ssqr, flat, fstage, rbuf, lsem, sems,
):
    c, t = lax.axis_index("ctx"), lax.axis_index("tp")
    q, core = lax.div(c, 2), lax.rem(c, 2)
    mate = q * 2 + (1 - core)
    blk = core * CHIPS + q
    prompts, tokens, width = x_ref.shape
    tiles = width // LANES
    states = init_hbm.shape[3]
    steps, batch = dx_ref.shape[:2]
    rows = batch * CTX
    heads = dt_ref.shape[1]

    barrier = pltpu.get_barrier_semaphore()
    for k in range(1, CTX):
        pl.semaphore_signal(barrier, inc=1, device_id=(lax.rem(c + k, CTX), t), device_id_type=MESH)
    for k in range(1, TP):
        pl.semaphore_signal(barrier, inc=1, device_id=(c, lax.rem(t + k, TP)), device_id_type=MESH)

    def lanes_of(j, size=LANES):
        return pl.ds(pl.multiple_of(j * size, size), size)

    def remote(src, dst, ssem, rsem, ctx=None, tp=None):
        return pltpu.make_async_remote_copy(
            src_ref=src, dst_ref=dst, send_sem=ssem, recv_sem=rsem,
            device_id=(c if ctx is None else ctx, t if tp is None else tp),
            device_id_type=MESH,
        )

    zed, why = lax.div(q, 2), lax.rem(q, 2)
    neighbour = (2 * zed + 1 - why) * 2 + core

    def device_of(chip):
        return chip * 2 + core

    def zed_at(k):
        return lax.rem(zed + k, PAIRS)

    def zed_from(k):
        return lax.rem(zed + PAIRS - k, PAIRS)

    taken = []

    def new(count=None):
        base = sum(taken)
        taken.append(count or 1)
        return sems.at[base] if count is None else lambda k: sems.at[base + k]

    def wait_sent(sem, ref):
        remote(ref, ref, sem, sem, ctx=mate).wait_send()

    def wait_got(sem, ref):
        remote(ref, ref, sem, sem, ctx=mate).wait_recv()

    rims, rimr = new(), new()
    decs, decr = new(3), new(3)
    sps, spn, spr, psr = new(3), new(3), new(3), new(3)
    d2s, d2r, dds, ddr, e2s, e2r = new(), new(CHIPS), new(), new(), new(), new(2)
    yos, yor, yds, ydr = new(), new(PAIRS), new(), new()
    zos, zor, zds, zdr = new(), new(PAIRS), new(), new()
    rs_, rr, yes_, yer = new(), new(PAIRS), new(), new(PAIRS)
    gns, gqs, gfs = new(), new(), new()
    gnr, gzr, gqr, gfr, qr, tr = [new(PARTS) for _ in range(6)]
    qs, ts = new(), new()
    assert sum(taken) == sems.shape[0]

    def load(at, src, dst):
        copy = pltpu.make_async_copy(src, dst, lsem.at[at])
        copy.start()
        return copy

    xcopy, bcopy = load(0, x_hbm, x_ref), load(1, bc_hbm, bc_ref)
    dcopies = [
        load(2, dx_hbm, dx_ref), load(3, dz_hbm, dz_ref), load(4, dbc_hbm, dbc_ref)
    ]
    icopy = load(5, init_hbm.at[:, blk], ibuf)
    zcopy, wcopy = load(6, z_hbm, zbuf), load(7, w_hbm, wbuf)

    hrow[...] = jnp.zeros_like(hrow)
    hrow[0:1, :heads] = jnp.exp(alog_ref[...])
    hrow[1:2, :heads] = dtb_ref[...]
    hrow[2:3, :heads] = dsk_ref[...]
    spread4[...] = jnp.zeros_like(spread4)
    for i in range(steps):
        spread4[i, :, :heads] = softplus(ddt_ref[i] + hrow[1:2, :heads])
    small[0] = sum(
        spread4[i] if i == 0 else pltpu.roll(spread4[i], heads * i, 1) for i in range(steps)
    )
    which = jnp.zeros((batch, LANES), F32)
    row_at = lax.broadcasted_iota(jnp.int32, (batch, LANES), 0)
    for r in range(batch):
        which = jnp.where(row_at == r, rp_ref[r].astype(F32), which)
    small[1] = which

    upto = lax.broadcasted_iota(jnp.int32, (tokens, tokens), 0)
    at_lane = lax.broadcasted_iota(jnp.int32, (tokens, tokens), 1)
    upper = jnp.where(upto <= at_lane, 1.0, 0.0)
    lower = upto >= at_lane
    hcol = jnp.concatenate([hrow[...], jnp.zeros((LANES - 8, LANES), F32)], 0).T
    rate_col, bias_col = hcol[:heads, 0:1], hcol[:heads, 1:2]
    lane_place = lax.broadcasted_iota(jnp.int32, (heads, tokens), 1) + c * tokens
    for s in range(prompts):
        live = lane_place < len_ref[s]
        step = jnp.where(live, softplus(dt_ref[s] + bias_col), 0.0)
        run = jnp.dot(-rate_col * step, upper, precision=HIGH, preferred_element_type=F32)
        runrows[s] = run
        both = jnp.concatenate([run, step, jnp.zeros((tokens - 2 * heads, tokens), F32)], 0)
        cols[s] = both.T
    first_half = lax.broadcasted_iota(jnp.int32, (tokens, LANES), 1) < LANES // 2
    ends = [cols[s][tokens - 1 :] for s in range(prompts)]
    ends = jnp.exp(jnp.concatenate(ends + [jnp.zeros((8 - prompts, LANES), F32)], 0))
    for j in range(tiles):
        dall[j] = jnp.where(first_half[:8], ends[:, 2 * j : 2 * j + 1], ends[:, 2 * j + 1 : 2 * j + 2])

    xcopy.wait()
    bcopy.wait()
    ends = [x_ref[s, tokens - 16 :, :].astype(F32)[8:] for s in range(prompts)]
    rimsend[:, :width] = jnp.concatenate(ends, 0).astype(BF16)
    ends = [bc_ref[s, tokens - 16 :, :].astype(F32)[8:] for s in range(prompts)]
    rimsend[:, width:] = jnp.concatenate(ends, 0).astype(BF16)
    pl.semaphore_wait(barrier, CTX - 1 + TP - 1)

    rim = remote(rimsend, rimrecv, rims, rimr, ctx=lax.rem(c + 1, CTX))
    pl.when(c != CTX - 1)(rim.start)
    half = pl.ds(pl.multiple_of((1 - core) * CHIPS, CHIPS), CHIPS)
    remote(dall.at[half], drecv, dds, ddr, ctx=mate).start()

    place = lax.broadcasted_iota(jnp.int32, (8, tokens), 1) + c * tokens
    slot = lax.broadcasted_iota(jnp.int32, (8, tokens), 0)
    tx, tbc = 0.0, 0.0
    for s in range(prompts):
        hit = (place == len_ref[s] - 3 + slot - 4 * s) & (slot >= 4 * s) & (slot < 4 * s + 3)
        pick = jnp.where(hit, 1.0, 0.0).astype(BF16)
        tx = tx + dot(pick, x_ref[s])
        tbc = tbc + dot(pick, bc_ref[s])
    tailx[...] = tx.astype(BF16)
    tailbc[...] = tbc.astype(BF16)

    for copy in dcopies:
        copy.wait()
    dxr[:, c] = dx_ref[:, :, lanes_of(blk)]
    dzr[:, c] = dz_ref[:, :, lanes_of(blk)]
    dbcr[:, c] = dbc_ref[...]
    smr[c] = small[...]
    txr[c] = tailx[:, lanes_of(blk)]
    tbr[c] = tailbc[...]

    def scatter_copies(k, source):
        to = lax.rem(c + k, CTX)
        their = lax.rem(to, 2) * CHIPS + lax.div(to, 2)
        at = lax.rem(c + CTX - k, CTX) if source else c
        pairs = (
            (dx_ref.at[:, :, lanes_of(their)], dxr.at[:, at]),
            (dz_ref.at[:, :, lanes_of(their)], dzr.at[:, at]),
            (tailx.at[:, lanes_of(their)], txr.at[at]),
        )
        return [
            remote(src, dst, decs(i), decr(i), ctx=to)
            for i, (src, dst) in enumerate(pairs)
        ]

    spread_refs = (dbc_ref, small, tailbc)

    def spread_to(at):
        return dbcr.at[:, at], smr.at[at], tbr.at[at]

    def spread_copies(k, source):
        if isinstance(k, int):
            to, at = neighbour, neighbour
        else:
            to, at = device_of(2 * zed_at(k) + why), device_of(2 * zed_from(k) + why)
        return [
            remote(src, dst, sps(i), spn(i) if isinstance(k, int) else spr(i), ctx=to)
            for i, (src, dst) in enumerate(zip(spread_refs, spread_to(at if source else c)))
        ]

    def relay_copies(k, source):
        at = device_of(2 * (zed_from(k) if source else zed) + 1 - why)
        return [
            remote(ref, ref, sps(i), spr(i), ctx=device_of(2 * zed_at(k) + why))
            for i, ref in enumerate(spread_to(at))
        ]

    def pass_copies(chip, source):
        at = chip * 2 + (1 - core if source else core)
        return [
            remote(ref, ref, sps(i), psr(i), ctx=mate)
            for i, ref in enumerate(spread_to(at))
        ]

    @pl.loop(1, CTX)
    def _(k):
        for copy in scatter_copies(k, False):
            copy.start()

    for copy in spread_copies(0, False):
        copy.start()

    @pl.loop(1, PAIRS)
    def _(k):
        for copy in spread_copies(k, False):
            copy.start()

    def entry_copy(k, source):
        to = zed_at(k)
        src, at = (zed, zed_from(k)) if source else (to, zed)
        return remote(
            retst.at[src], erecv.at[at], rs_, rr(k), ctx=device_of(2 * to + why)
        )

    icopy.wait()
    for s in range(prompts):
        est[s] = ibuf[s].T
        retst[0, s] = est[s].astype(BF16)

    @pl.when(zed != 0)
    def _():
        entry_copy(PAIRS - zed, False).start()

    @pl.when(c != 0)
    def _():
        rim.wait_recv()
        rimf[...] = rimrecv[...].astype(F32)

    @pl.when(c == 0)
    def _():
        rimf[...] = jnp.zeros_like(rimf)
        for s in range(prompts):
            for k in range(3):
                at = 8 * s + 5 + k
                rimf[at : at + 1, :width] = icx_ref[k].astype(F32)[s : s + 1]
                rimf[at : at + 1, width:] = icbc_ref[k].astype(F32)[s : s + 1]

    def conv(rim_rows, body, taps, bias):
        padded = jnp.concatenate([rim_rows, body], 0)
        total = bias
        for k in range(4):
            total = total + taps[k] * padded[5 + k : 5 + k + body.shape[0]]
        return silu(total)

    bc_taps = [cbc_ref[k] for k in range(4)]
    for s in range(prompts):
        act = conv(rimf[8 * s : 8 * s + 8, width:], bc_ref[s].astype(F32), bc_taps, bbc_ref[...])
        b, cc = act[:, :states], act[:, states:]
        bt = b.T
        high, low = split(bt)
        bthl[s] = jnp.concatenate([high, low], 1)
        chl[s] = jnp.concatenate(split(cc), 0)
        scores = jnp.dot(cc, bt, precision=HIGH, preferred_element_type=F32)
        scs[s] = jnp.where(lower, scores, 0.0)

    def columns(s, j):
        return pltpu.roll(cols[s], lax.rem(tokens - 2 * j, tokens), 1)

    def per_lane(row, j):
        rolled = pltpu.roll(hrow[...], lax.rem(LANES - 2 * j, LANES), 1)[row : row + 1]
        return jnp.where(first_half[:1], rolled[:, 0:1], rolled[:, 1:2])

    def taps_of(lanes):
        taps = cx_ref[:, lanes]
        return [taps[k : k + 1] for k in range(4)]

    def own_part(j, i, out):
        lanes = lanes_of(j)
        taps, skip = taps_of(lanes), per_lane(2, j)
        for s in range(prompts):
            body = x_ref[s, :, lanes].astype(F32)
            xv = conv(rimf[8 * s : 8 * s + 8, lanes], body, taps, bx_ref[:, lanes])
            col = columns(s, j)
            r = jnp.where(first_half, col[:, 0:1], col[:, 1:2])
            step = jnp.where(first_half, col[:, heads : heads + 1], col[:, heads + 1 : heads + 2])
            end = r[tokens - 1 : tokens]
            v = xv * step
            vp[s, j] = v
            er[s, j] = jnp.exp(r)
            yacc[s, j] = skip * xv
            high, low = split(v * jnp.exp(end - r))
            out[i, s] = dot(bthl[s], jnp.concatenate([high, high], 0)) + dot(
                bthl[s, :, :tokens], low
            )

    is_first = core == 0

    def state_copy(i):
        return remote(osend.at[i], orecv.at[i], d2s, d2r(i), ctx=mate)

    def decays(s, i):
        return dall[core * CHIPS + i, s : s + 1], drecv[i, s : s + 1]

    def pair_copy(at):
        return remote(ysend.at[at], yrecv.at[at], yos, yor(at), ctx=neighbour)

    def zed_copy(k, source, refs, ssem, rsem):
        to = zed_at(k)
        src, at = (zed, zed_from(k)) if source else (to, zed)
        return remote(refs[0].at[src], refs[1].at[at], ssem, rsem, ctx=device_of(2 * to + why))

    def zed_state(k, source):
        return zed_copy(k, source, (zsend, zrecv), zos, zor(k))

    def zed_decay(k):
        return zed_copy(k, False, (zdsend, zdrecv), zds, zdr)

    def block_of(n):
        at = lax.rem(zed + n, PAIRS)
        return at, 2 * at + jnp.where(n <= PAIRS, 1 - why, why)

    is_low = why == 0

    def combine(n):
        at, i = block_of(n)
        state_copy(i).wait_recv()
        for s in range(prompts):
            down, theirs = decays(s, i)
            a = jnp.where(is_first, theirs, 1.0)
            b = jnp.where(is_first, 1.0, down)
            ochip[at, s] = a * oown[i, s] + b * orecv[i, s]

        @pl.when(n <= PAIRS)
        def _():
            for s in range(prompts):
                ysend[at, s] = ochip[at, s].astype(BF16)
            pair_copy(at).start()

    def quad(m):
        at = zed_at(m)
        pair_copy(at).wait_recv()
        for s in range(prompts):
            down, theirs = dchip[at, s : s + 1], ydrecv[at, s : s + 1]
            a = jnp.where(is_low, theirs, 1.0)
            b = jnp.where(is_low, 1.0, down)
            zsend[at, s] = (a * ochip[at, s] + b * yrecv[at, s].astype(F32)).astype(BF16)

    def quad_send(m):
        quad(m)
        zed_state(m, False).start()

    wait_got(ddr, drecv)
    for at in range(PAIRS):
        for ref, i in ((dchip, 2 * at + why), (ydsend, 2 * at + 1 - why)):
            ref[at] = dall[core * CHIPS + i] * drecv[i]
    pair_decays = remote(ydsend, ydrecv, yds, ydr, ctx=neighbour)
    pair_decays.start()

    @pl.loop(1, CHIPS + 1)
    def _(n):
        i = block_of(n)[1]
        own_part((1 - core) * CHIPS + i, i, osend)
        own_part(core * CHIPS + i, i, oown)
        state_copy(i).start()

        @pl.when(n > 1)
        def _():
            combine(n - 1)

        @pl.when(n == 3)
        def _():
            for copy in spread_copies(0, True):
                copy.wait_recv()

            @pl.loop(1, PAIRS)
            def _(k):
                for copy in relay_copies(k, False):
                    copy.start()

            pair_decays.wait_recv()
            zdsend[...] = dchip[...] * ydrecv[...]

            @pl.loop(1, PAIRS)
            def _(k):
                zed_decay(k).start()

        @pl.when(n > PAIRS + 2)
        def _():
            quad_send(n - PAIRS - 2)

    combine(CHIPS)

    def inside(j):
        for s in range(prompts):
            col = columns(s, j)
            mixing = []
            for h in range(2):
                row = runrows[s, pl.ds(2 * j + h, 1), :]
                gap = jnp.minimum(col[:, h : h + 1] - row, 0.0)
                mixing.append((jnp.exp(gap) * scs[s]).astype(BF16))
            both = jnp.concatenate(mixing, 1)
            v = vp[s, j]
            total = yacc[s, j]
            stacked = jnp.concatenate([jnp.where(first_half, v, 0.0), jnp.where(first_half, 0.0, v)], 0)
            for part in split(stacked):
                total = total + dot(both, part)
            yacc[s, j] = total

    cuts = (0, 4, 8, 10)
    pl.loop(0, cuts[1])(inside)
    quad_send(PAIRS - 1)
    pl.loop(cuts[1], cuts[2])(inside)
    quad(PAIRS)
    zrecv[zed] = zsend[zed]
    zdrecv[zed] = zdsend[zed]

    for copy in pass_copies(q, False):
        copy.start()

    for i, ref in enumerate(spread_to(pl.ds(0, 2 * (PAIRS - 1)))):
        wait_got(spr(i), ref)

    @pl.loop(0, CHIPS)
    def _(chip):
        @pl.when(chip != q)
        def _():
            for copy in pass_copies(chip, False):
                copy.start()

    wait_got(zdr, zdrecv.at[: PAIRS - 1])

    @pl.loop(0, PAIRS)
    def _(p):
        @pl.when(p > 0)
        def _():
            for s in range(prompts):
                retst[p, s] = est[s].astype(BF16)

        @pl.when((p > 0) & (p != zed))
        def _():
            entry_copy(lax.rem(p - zed + PAIRS, PAIRS), False).start()

        @pl.when(p != zed)
        def _():
            zed_state(lax.rem(zed - p + PAIRS, PAIRS), True).wait_recv()

        for s in range(prompts):
            est[s] = zdrecv[p, s : s + 1] * est[s] + zrecv[p, s].astype(F32)

    erecv[zed] = retst[zed]

    def entry_to_neighbour(at):
        return remote(yesend.at[at], yerecv.at[at], yes_, yer(at), ctx=neighbour)

    def mate_copy(i, group):
        return remote(e2send.at[i], e2recv.at[i], e2s, e2r(group), ctx=mate)

    def for_cores(i, s, e):
        down, theirs = decays(s, i)
        e2send[i, s] = jnp.where(is_first, down * e + oown[i, s], e)
        emine[i, s] = jnp.where(is_first, e, theirs * e + orecv[i, s])

    def entry_step(at):
        i = 2 * at + why
        entries = []
        for s in range(prompts):
            down, theirs = dchip[at, s : s + 1], ydrecv[at, s : s + 1]
            e = erecv[at, s].astype(F32)
            yesend[at, s] = jnp.where(is_low, down * e + ochip[at, s], e).astype(BF16)
            entries.append(jnp.where(is_low, e, theirs * e + yrecv[at, s].astype(F32)))
        entry_to_neighbour(at).start()
        for s in range(prompts):
            for_cores(i, s, entries[s])
        mate_copy(i, 0).start()

    entry_step(zed)

    others = (dxr.at[:, : CTX - 1], dzr.at[:, : CTX - 1], txr.at[: CTX - 1])
    for i, ref in enumerate(others):
        wait_got(decr(i), ref)
    for i, ref in enumerate(spread_to(pl.ds(0, CHIPS))):
        wait_got(psr(i), ref)

    part_steps = steps // PARTS
    part = part_steps * rows

    def slab(chip, which, h):
        at = which * CHIPS + chip
        return gbuf.at[lax.div(at, 2), h * part : (h + 1) * part, lanes_of(lax.rem(at, 2))]

    def to_neighbour(h, source):
        at = 2 * zed + (1 - why if source else why)
        return remote(slab(q, core, h), slab(at, core, h), gns, gnr(h), ctx=neighbour)

    def gather_copy(k, h, source):
        at = 2 * zed_from(k) + why if source else q
        to = device_of(2 * zed_at(k) + why)
        return remote(slab(q, core, h), slab(at, core, h), gns, gzr(h), ctx=to)

    def relay_copy(k, h, source):
        piece = slab(2 * (zed_from(k) if source else zed) + 1 - why, core, h)
        to = device_of(2 * zed_at(k) + why)
        return remote(piece, piece, gqs, gqr(h), ctx=to)

    def forward_copy(chip, h, source):
        piece = slab(chip, 1 - core if source else core, h)
        return remote(piece, piece, gfs, gfr(h), ctx=mate)

    def square_copy(k, h, source):
        at = lax.rem(c + CTX - k, CTX) if source else c
        to = lax.rem(c + k, CTX)
        return remote(ssqs.at[h], ssqr.at[h, at], qs, qr(h), ctx=to)

    def send_along(h):
        @pl.loop(1, PAIRS)
        def _(k):
            gather_copy(k, h, False).start()

    def send_rows(h):
        to_neighbour(h, False).start()
        if h == 0:
            send_along(h)
        forward_copy(q, h, False).start()

        @pl.loop(1, CTX)
        def _(k):
            square_copy(k, h, False).start()

    def relay_rows(h):
        to_neighbour(h, True).wait_recv()

        @pl.loop(1, PAIRS)
        def _(k):
            relay_copy(k, h, False).start()

        if h + 1 < PARTS:
            send_along(h + 1)
        forward_copy(2 * zed + 1 - why, h, False).start()

    lanes = lanes_of(blk)
    taps, bias, gain = taps_of(lanes), bx_ref[:, lanes], gain_ref[:, lanes]
    rate, skip = per_lane(0, blk), per_lane(2, blk)
    second = smr[:, 1].reshape(rows, LANES)[:, 0:1] > 0.5
    sizes = smr[:, 0].reshape(rows, LANES)
    rolled = pltpu.roll(sizes, lax.rem(LANES - 2 * blk, LANES), 1)

    def window(ref):
        out = ref[0].astype(F32)
        for i in range(1, CTX):
            out = out + ref[i].astype(F32)
        return [jnp.where(second, out[4 + k : 5 + k], out[k : k + 1]) for k in range(3)]

    def flat_rows(ref, i):
        return ref[i].astype(F32).reshape(rows, ref.shape[3])

    seq_x = window(txr) + [flat_rows(dxr, i) for i in range(steps)]
    seq_b = window(tbr) + [flat_rows(dbcr, i) for i in range(steps)]

    def taps_on(seq, i, weights, total):
        for k in range(4):
            total = total + weights[k] * seq[i + k]
        return silu(total)

    final = [split(est[s]) for s in range(prompts)]
    bs, us = [], []
    grown = 1.0
    row8 = lax.broadcasted_iota(jnp.int32, (8, LANES), 0)
    for i in range(steps):
        xd = taps_on(seq_x, i, taps, bias)
        bcd = taps_on(seq_b, i, bc_taps, bbc_ref[...])
        cd = bcd[:, states:]
        chigh, clow = split(cd)
        at = heads * i
        step = jnp.where(first_half, rolled[:, at : at + 1], rolled[:, at + 1 : at + 2])
        keep = jnp.exp(-rate * step)
        grown = grown * keep
        bs.append(bcd[:, :states])
        us = [keep * u for u in us] + [step * xd]
        y0 = [
            dot(chigh, high) + dot(clow, high) + dot(chigh, low) for high, low in final
        ]
        yd = grown * jnp.where(second, y0[1], y0[0]) + skip * xd
        for b, u in zip(bs, us):
            yd = yd + u * jnp.sum(b * cd, axis=1, keepdims=True)
        m = yd * silu(flat_rows(dzr, i))
        if i % part_steps == 0:
            squares = jnp.zeros((8, rows), F32)
        squares = squares + lax.dot_general(
            jnp.where(row8 == i, 1.0, 0.0), m * m, (((1,), (1,)), ((), ())),
            precision=HIGH, preferred_element_type=F32,
        )
        gbuf[lax.div(blk, 2), i * rows : (i + 1) * rows, lanes_of(lax.rem(blk, 2))] = (
            m * gain
        ).astype(BF16)
        if i % part_steps == part_steps - 1:
            ssqs[i // part_steps] = squares
            ssqr[i // part_steps, c] = squares
            send_rows(i // part_steps)

    pl.loop(cuts[2], cuts[3])(inside)
    for h in range(PARTS):
        relay_rows(h)
        if h + 1 < PAIRS:
            entry_copy(h + 1, True).wait_recv()
            entry_step(zed_from(h + 1))
            pl.loop(cuts[3] + 2 * h, cuts[3] + 2 * h + 2)(inside)

    zcopy.wait()
    ssqp[...] = jnp.zeros_like(ssqp)

    def finish(s, j, entry):
        high, low = split(entry)
        carried = dot(chl[s], high)
        carried = carried[:tokens] + carried[tokens:] + dot(chl[s, :tokens], low)
        y = yacc[s, j] + carried * er[s, j]
        m = y * silu(zbuf[s, :, lanes_of(j)].astype(F32))
        yacc[s, j] = m
        ssqp[s] += m * m

    def finish_mine(i):
        for s in range(prompts):
            finish(s, core * CHIPS + i, emine[i, s])

    def own_column():
        @pl.loop(0, PAIRS)
        def _(k):
            finish_mine(2 * zed_from(k) + why)

    def other_column():
        @pl.loop(0, PAIRS)
        def _(k):
            at = zed_from(k)
            i = 2 * at + 1 - why
            entry_to_neighbour(at).wait_recv()
            for s in range(prompts):
                for_cores(i, s, yerecv[at, s].astype(F32))
            mate_copy(i, 1).start()
            finish_mine(i)

    def other_core(group, column):
        wait_got(e2r(group), e2recv.at[:PAIRS])

        @pl.loop(0, PAIRS)
        def _(k):
            i = 2 * k + column
            for s in range(prompts):
                finish(s, (1 - core) * CHIPS + i, e2recv[i, s])

    wcopy.wait()
    pair, groups = 2 * LANES, CHIPS // 2
    share = rows // TP

    def projected(which, h):
        total = 0.0
        for g in range(groups):
            at = which * groups + g
            w = wbuf[pl.ds(pl.multiple_of(at * pair, pair), pair), :]
            total = total + dot(gbuf[at, h * part : (h + 1) * part], w)
        return total

    def rows_of(at):
        return pl.ds(pl.multiple_of(at * share, share), share)

    def sum_copy(k, h, source):
        to = lax.rem(t + k, TP)
        at = lax.rem(t + TP - k, TP) if source else t
        these = slice(h * part_steps, (h + 1) * part_steps)
        return remote(
            fstage.at[these, rows_of(to), :], rbuf.at[at, these], ts, tr(h), tp=to
        )

    for h in range(PARTS):

        three = gbuf.at[0, : (PAIRS - 1) * part // 2]
        wait_got(gzr(h), three)

        @pl.loop(1, PAIRS)
        def _(k):
            forward_copy(2 * zed_from(k) + why, h, False).start()

        wait_got(gqr(h), three)

        @pl.loop(1, PAIRS)
        def _(k):
            forward_copy(2 * zed_from(k) + 1 - why, h, False).start()

        flat[...] = projected(core, h)

        if h == 0:
            own_column()
        if h == 1:
            other_core(0, why)
        wait_got(gfr(h), gbuf.at[0])
        wait_got(qr(h), ssqr.at[h, : CTX - 1])

        squares = ssqr[h, 0]
        for i in range(1, CTX):
            squares = squares + ssqr[h, i]
        scale = lax.rsqrt(squares * (1.0 / width) + 1e-5)
        scale = jnp.concatenate([scale, jnp.zeros((rows - 8, rows), F32)], 0).T
        total = flat[...] + projected(1 - core, h)
        for i in range(part_steps):
            at = h * part_steps + i
            fstage[at] = (total[i * rows : (i + 1) * rows] * scale[:, at : at + 1]).astype(BF16)

        @pl.loop(1, TP)
        def _(k):
            sum_copy(k, h, False).start()

        if h == FINISH[0]:
            other_column()
        if h == FINISH[1]:
            other_core(1, 1 - why)

    rbuf[t] = fstage[:, rows_of(t), :]

    for s in range(prompts):
        mean = jnp.sum(ssqp[s], axis=1, keepdims=True) * (1.0 / width)
        ssqp[s] = jnp.broadcast_to(lax.rsqrt(mean + 1e-5), ssqp.shape[1:])

    outs = []
    for s in range(prompts):

        @pl.loop(0, tiles)
        def _(j):
            gain = gain_ref[:, lanes_of(j)]
            pre_ref[s, :, lanes_of(j)] = (yacc[s, j] * ssqp[s] * gain).astype(BF16)

        outs.append(pltpu.make_async_copy(pre_ref.at[s], pre_hbm.at[s], lsem.at[s]))
        outs[s].start()

    pl.when(c != CTX - 1)(rim.wait_send)
    wait_sent(dds, drecv)

    for i, ref in enumerate(others):
        wait_sent(decs(i), ref)
    for i, ref in enumerate(spread_to(pl.ds(0, CTX - 1))):
        wait_sent(sps(i), ref)
    three = slice(0, PAIRS - 1)
    for sem, ref in (
        (d2s, osend), (e2s, e2send), (yos, ysend), (yds, ydsend), (yes_, yesend),
        (zos, zsend.at[three]), (zds, zdsend.at[three]), (rs_, retst.at[three]),
        (gns, gbuf.at[:2]), (gqs, gbuf.at[three, : steps * rows // 2]), (gfs, gbuf.at[:4]),
        (qs, ssqr.at[:, : CTX - 1]),
    ):
        wait_sent(sem, ref)

    for h in range(PARTS):
        wait_got(tr(h), rbuf.at[: TP - 1, h * part_steps : (h + 1) * part_steps])

    total = rbuf[0].astype(F32)
    for i in range(1, TP):
        total = total + rbuf[i].astype(F32)
    lay_ref[...] = total.astype(BF16)

    wait_sent(ts, rbuf.at[: TP - 1])

    for copy in outs:
        copy.wait()


def hand_on(a_hbm, b_hbm, a_out, b_out, abuf, bbuf, isem, osem):
    pieces = [(b_hbm, bbuf, b_out)]
    half = a_hbm.shape[1] // 2
    for s in range(a_hbm.shape[0]):
        for r in range(2):
            at = (s, slice(r * half, (r + 1) * half))
            pieces.append((a_hbm.at[at], abuf.at[at], a_out.at[at]))
    into = [pltpu.make_async_copy(a, b, isem.at[i]) for i, (a, b, _) in enumerate(pieces)]
    out = [pltpu.make_async_copy(b, o, osem.at[i]) for i, (_, b, o) in enumerate(pieces)]
    for copy in into:
        copy.start()
    for first, then in zip(into, out):
        first.wait()
        then.start()
    for copy in out:
        copy.wait()


def shards(
    inner_x, gate_z, proj_bc, dt_raw, a_log, dt_bias, d_skip, conv_x, conv_bc, bias_x, bias_bc,
    norm_gain, init_state, init_conv_x, init_conv_bc, lengths, dec_x, dec_z, dec_bc, dec_dt,
    row_prompt, w_out,
):
    prompts, tokens, width = inner_x.shape
    bc_width = proj_bc.shape[3]
    states = bc_width // 2
    heads = dt_raw.shape[1]
    steps, batch = dec_x.shape[:2]
    out_width = w_out.shape[1]
    tiles = width // LANES
    rows = batch * CTX
    vm = pl.BlockSpec(memory_space=pltpu.VMEM)
    hb = pl.BlockSpec(memory_space=pltpu.HBM)
    sm = pl.BlockSpec(memory_space=pltpu.SMEM)
    dma = pltpu.SemaphoreType.DMA
    V = pltpu.VMEM
    state = (CHIPS, prompts, states, LANES)
    pairs = (PAIRS, prompts, states, LANES)
    tile = (prompts, tiles, tokens, LANES)
    scratch = [
        V((prompts, tokens, width), BF16),
        V((prompts, tokens, bc_width), BF16),
        V((steps, batch, width), BF16),
        V((steps, batch, width), BF16),
        V((steps, batch, bc_width), BF16),
        V((prompts, tokens, width), BF16),
        V((prompts, tokens, width), BF16),
        V((prompts, LANES, states), F32),
        V((width, out_width), BF16),
        V((8 * prompts, width + bc_width), BF16),
        V((8 * prompts, width + bc_width), BF16),
        V((8 * prompts, width + bc_width), F32),
        V((8, width), BF16),
        V((8, bc_width), BF16),
        V((2, batch, LANES), F32),
        V((steps, batch, LANES), F32),
        V((8, LANES), F32),
        V((steps, CTX, batch, LANES), BF16),
        V((steps, CTX, batch, LANES), BF16),
        V((steps, CTX, batch, bc_width), BF16),
        V((CTX, 2, batch, LANES), F32),
        V((CTX, 8, LANES), BF16),
        V((CTX, 8, bc_width), BF16),
        V((prompts, heads, tokens), F32),
        V((prompts, tokens, tokens), F32),
        V((prompts, states, 2 * tokens), BF16),
        V((prompts, 2 * tokens, states), BF16),
        V((prompts, tokens, tokens), F32),
        V((tiles, 8, LANES), F32),
        V((CHIPS, 8, LANES), F32),
        *[V((PAIRS, 8, LANES), F32) for _ in range(5)],
        V(state, F32),
        V(state, F32),
        V(state, F32),
        V(pairs, BF16),
        V(pairs, BF16),
        V(pairs, F32),
        V(pairs, BF16),
        V(pairs, BF16),
        V((prompts, states, LANES), F32),
        V(pairs, BF16),
        V(pairs, BF16),
        V(pairs, BF16),
        V(pairs, BF16),
        V(state, F32),
        V(state, F32),
        V(state, F32),
        V(tile, F32),
        V(tile, F32),
        V(tile, F32),
        V((prompts, tokens, LANES), F32),
        V((tiles // 2, steps * rows, 2 * LANES), BF16),
        V((PARTS, 8, rows), F32),
        V((PARTS, CTX, 8, rows), F32),
        V((steps * rows // PARTS, out_width), F32),
        V((steps, rows, out_width), BF16),
        V((TP, steps, rows // TP, out_width), BF16),
        dma((8,)),
        dma((87,)),
    ]
    prefill, layer = pl.pallas_call(
        kernel,
        out_shape=(
            jax.ShapeDtypeStruct((prompts, tokens, width), BF16),
            jax.ShapeDtypeStruct((steps, rows // TP, out_width), BF16),
        ),
        in_specs=[hb, hb, hb, *[vm] * 9, hb, vm, vm, sm, hb, hb, hb, vm, sm, hb],
        out_specs=(hb, vm),
        scratch_shapes=scratch,
        compiler_params=pltpu.CompilerParams(
            collective_id=0, has_side_effects=True, vmem_limit_bytes=60 * 2**20
        ),
        name="mixer",
    )(
        inner_x, proj_bc.reshape(prompts, tokens, bc_width), gate_z, dt_raw,
        a_log[None], dt_bias[None], d_skip[None], conv_x, conv_bc, bias_x[None], bias_bc,
        norm_gain[None], init_state.reshape(prompts, tiles, LANES, states),
        jnp.transpose(init_conv_x, (1, 0, 2)),
        jnp.transpose(init_conv_bc, (1, 2, 0, 3)).reshape(3, prompts, bc_width),
        lengths, dec_x, dec_z, dec_bc.reshape(steps, batch, bc_width),
        jnp.transpose(dec_dt, (0, 2, 1)), row_prompt, w_out,
    )
    halves = (prompts, tokens, width), (steps, rows // TP, out_width)
    return pl.pallas_call(
        hand_on,
        out_shape=tuple(jax.ShapeDtypeStruct(shape, BF16) for shape in halves),
        in_specs=[hb, hb],
        out_specs=(hb, hb),
        scratch_shapes=[*[V(shape, BF16) for shape in halves], dma((5,)), dma((5,))],
        name="results",
    )(prefill, layer)


def solution(mesh):
    ctx, tp = "ctx", "tp"
    placed = (
        P(None, ctx, tp), P(None, ctx, tp), P(None, ctx, tp, None), P(None, tp, ctx),
        P(tp), P(tp), P(tp), P(None, tp), P(None, tp, None), P(tp), P(tp, None), P(tp),
        P(None, tp, None, None), P(None, None, tp), P(None, None, tp, None), P(),
        P(None, ctx, tp), P(None, ctx, tp), P(None, ctx, tp, None), P(None, tp, ctx),
        P(ctx), P(tp, ctx),
    )
    return jax.shard_map(
        shards,
        mesh=mesh,
        in_specs=placed,
        out_specs=(P(None, ctx, tp), P(None, tp, ctx)),
        check_vma=False,
    )
```
